32 devices in a mesh: gx: 4 (over y, x), gy: 8 (over z, core).
Axes of the slice: x: 2, y: 2, z: 4, core: 2. Of those that a mesh axis runs over, the one named last changes fastest.
Arguments:
- features: bfloat16 [131072, 256], P(('gx', 'gy')), may hold values from -0.375 to 0.375
- inv_width: bfloat16 [131072], P(('gx', 'gy')), may hold values from 0.29882812 to 3
- start_block: float32 [32, 131072], P(None, ('gx', 'gy')), may hold values from -6 to 6
- neighbour_ids: int32 [1024, 16], P(('gx', 'gy')), may hold values from 0 to 1023, as said below
- slot_mask: int32 [1024, 16], P(('gx', 'gy')), may hold values from 0 to 1
Outputs:
- basis: float32 [32, 131072], P(None, ('gx', 'gy'))
- factor: float32 [32, 32], replicated
The draws below stay inside these ranges and needn't reach their ends.
Inputs may be any that keep to these rules, and one draw needn't show every extreme that they name: `neighbour_ids`: entry j = 0 of every band b is b itself with slot_mask 1; wherever slot_mask is 0 the entry is b. Band c is held by device c // 32 (devices in the order gx, then gy). The entries with mask 1 of one device's bands name at most 2 distinct bands held by any one other device, and every device names exactly 2 bands of some other device.
All inputs are finite; a program needn't handle non-finite values.
Results may differ from the reference program's by a relative error of at most 0.0025.
Values may be sent and summed in bfloat16 or wider, within the bound.
No kernel may reach another device: no remote copies, remote signals or barrier semaphores. Data moves between devices by JAX's collectives and lax.ppermute only.
A program may use at most 128 MiB of HBM per device.

```python
import math
import jax
import jax.numpy as jnp
from jax import lax

F = 256
VECTORS = 32
BAND = 128
SLOTS = 16
DEGREE = 4
BANDS_DEV = 32
PEERS = 31
BANDS = 1024
ROWS = 131072


def neighbour_tables(key):
    count_dev = BANDS // BANDS_DEV
    free_slots = BANDS_DEV * (SLOTS - 1)
    base = jax.random.fold_in(key, 4711)
    subkeys = jax.random.split(base, 9)
    device_keys = jax.random.split(subkeys[0], count_dev)
    offsets = jax.vmap(lambda subkey: jax.random.permutation(subkey, count_dev - 1)[:PEERS] + 1)(device_keys)
    device_ids = jnp.arange(count_dev, dtype=jnp.int32)[:, None]
    sources = (device_ids + offsets) % count_dev
    first_band = jax.random.randint(subkeys[1], (count_dev, PEERS), 0, BANDS_DEV)
    second_band = (first_band + jax.random.randint(subkeys[2], (count_dev, PEERS), 1, BANDS_DEV)) % BANDS_DEV
    has_second = jax.random.randint(subkeys[3], (count_dev, PEERS), 0, 2)
    has_second = has_second.at[:, 0].set(1)
    pool_first = sources * BANDS_DEV + first_band
    pool_second = sources * BANDS_DEV + second_band
    local_pick = device_ids * BANDS_DEV + jax.random.randint(subkeys[4], (count_dev, free_slots), 0, BANDS_DEV)
    head_ids = jnp.stack([pool_first, jnp.where(has_second == 1, pool_second, local_pick[:, :PEERS])], axis=2)
    head_ids = head_ids.reshape(count_dev, 2 * PEERS)
    head_forced = jnp.stack([jnp.ones_like(has_second), has_second], axis=2).reshape(count_dev, 2 * PEERS)
    tail_count = free_slots - 2 * PEERS
    extra_peer = jax.random.randint(subkeys[5], (count_dev, tail_count), 0, PEERS)
    extra_pool = jnp.take_along_axis(pool_first, extra_peer, axis=1)
    use_pool = jax.random.randint(subkeys[6], (count_dev, tail_count), 0, 2)
    tail_ids = jnp.where(use_pool == 1, extra_pool, local_pick[:, 2 * PEERS:])
    entries = jnp.concatenate([head_ids, tail_ids], axis=1)
    forced = jnp.concatenate([head_forced, jnp.zeros((count_dev, tail_count), jnp.int32)], axis=1)
    chance = jax.random.randint(subkeys[7], (count_dev, free_slots), 0, 4)
    kept_slots = jnp.where((forced == 1) | (chance > 0), 1, 0)
    shuffle_keys = jax.random.split(subkeys[8], count_dev)
    shuffles = jax.vmap(lambda subkey: jax.random.permutation(subkey, free_slots))(shuffle_keys)
    entries = jnp.take_along_axis(entries, shuffles, axis=1).reshape(BANDS, SLOTS - 1)
    kept_slots = jnp.take_along_axis(kept_slots, shuffles, axis=1).reshape(BANDS, SLOTS - 1)
    own_bands = jnp.arange(BANDS, dtype=jnp.int32)[:, None]
    entries = jnp.where(kept_slots == 1, entries, own_bands)
    ids_table = jnp.concatenate([own_bands, entries], axis=1).astype(jnp.int32)
    mask_table = jnp.concatenate([jnp.ones((BANDS, 1), jnp.int32), kept_slots], axis=1).astype(jnp.int32)
    return (ids_table, mask_table)


def draw_neighbour_ids(key, part):
    return neighbour_tables(key)[0]


def draw_slot_mask(key, part):
    return neighbour_tables(key)[1]


def steps_of(own_key, extent, pieces, least, largest):
    def one(axis_at, shards_of):
        steps = jax.random.uniform(jax.random.fold_in(jax.random.fold_in(own_key, 6), axis_at), (shards_of,), jnp.float32, least / len(pieces), largest / len(pieces))
        return jnp.repeat(jnp.exp(steps), extent[axis_at] // shards_of).reshape((-1,) + (1,) * (len(extent) - axis_at - 1))

    loudness = one(*pieces[0])
    for cut in pieces[1:]:
        loudness = loudness * one(*cut)
    return loudness


def bell_draw(rng, dims, width, limit, cuts=(), kind=jnp.bfloat16):
    result = width * jax.random.normal(rng, dims, jnp.float32)
    if cuts:
        result = result * steps_of(rng, dims, cuts, -0.22, 0.18)
    return jnp.clip(result, -limit, limit).astype(kind)


def setup_inputs(seed: int = 0) -> dict:
    key_of = jax.random.split(jax.random.key(seed), 6)
    features = bell_draw(key_of[0], (ROWS, F), (F ** -0.5), 0.375, ((0, 32),))
    inv_width = jnp.clip(jnp.exp(math.log(3.0) - 2.306499 * jax.random.uniform(key_of[1], (ROWS,), jnp.float32) ** steps_of(key_of[1], (ROWS,), ((0, 32),), -0.2, 0.2)), 0.29882812, 3.0).astype(jnp.bfloat16)
    start_block = bell_draw(key_of[2], (VECTORS, ROWS), 1.0, 6.0, ((1, 32),), jnp.float32)
    neighbour_ids = draw_neighbour_ids(jax.random.fold_in(key_of[5], 71), 0)
    slot_mask = draw_slot_mask(jax.random.fold_in(key_of[5], 71), 0)
    return {"features": features, "inv_width": inv_width, "start_block": start_block, "neighbour_ids": neighbour_ids, "slot_mask": slot_mask}


LOW_EDGE = 0.2
HIGH_EDGE = 2.0

def chebyshev_terms():
    centre = 0.5 * (LOW_EDGE + HIGH_EDGE)
    halfwidth = 0.5 * (HIGH_EDGE - LOW_EDGE)
    anchor = -centre / halfwidth
    values = [1.0, anchor]
    for repeat in range(DEGREE - 1):
        values.append(2.0 * anchor * values[-1] - values[-2])
    return (centre, halfwidth, values)

def reference(features, inv_width, start_block, neighbour_ids, slot_mask):
    groups = BANDS // BANDS_DEV
    feature_bands = features.reshape(BANDS, BAND, F)
    width_bands = inv_width.reshape(BANDS, BAND).astype(jnp.float32)
    squares = lax.optimization_barrier(jnp.sum(jnp.square(feature_bands.astype(jnp.float32)), axis=-1))

    def grouped(stacked):
        return stacked.reshape((groups, BANDS_DEV) + stacked.shape[1:])

    def build(inputs):
        rows_block, width_block, square_block, ids_block, mask_block = inputs
        nearby = jnp.take(feature_bands, ids_block, axis=0).astype(jnp.float32)
        inner = jnp.einsum('brf,bjsf->bjrs', rows_block.astype(jnp.float32), nearby, precision=lax.Precision.HIGHEST)
        near_sq = jnp.take(squares, ids_block, axis=0)
        near_width = jnp.take(width_bands, ids_block, axis=0)
        distance = square_block[:, None, :, None] + near_sq[:, :, None, :] - 2.0 * inner
        spread = width_block[:, None, :, None] * near_width[:, :, None, :]
        weights = mask_block.astype(jnp.float32)[:, :, None, None] * jnp.exp(-distance * spread)
        return (weights.astype(jnp.bfloat16), lax.optimization_barrier(jnp.sum(weights, axis=(1, 3))))
    tiles, degree = lax.map(build, (grouped(feature_bands), grouped(width_bands), grouped(squares), grouped(neighbour_ids), grouped(slot_mask)))
    root_inv = 1.0 / jnp.sqrt(degree.reshape(BANDS, BAND))
    ids_grouped = grouped(neighbour_ids)

    def graph(block):
        scaled = (root_inv[:, None, :] * block).astype(jnp.bfloat16)

        def apply_tiles(inputs):
            tile_block, ids_block = inputs
            nearby = jnp.take(scaled, ids_block, axis=0).astype(jnp.float32)
            return jnp.einsum('bjrs,bjks->bkr', tile_block.astype(jnp.float32), nearby, precision=lax.Precision.HIGHEST)
        mixed = lax.map(apply_tiles, (tiles, ids_grouped)).reshape(BANDS, VECTORS, BAND)
        return root_inv[:, None, :] * mixed
    centre, halfwidth, values = chebyshev_terms()

    def shifted(block):
        return ((1.0 - centre) * block - graph(block)) / halfwidth
    previous = start_block.reshape(VECTORS, BANDS, BAND).transpose(1, 0, 2)
    current = shifted(previous) / values[1]
    for power in range(1, DEGREE):
        following = 2.0 * values[power] / values[power + 1] * shifted(current) - values[power - 1] / values[power + 1] * previous
        previous, current = (current, following)
    gram = jnp.einsum('bkr,bmr->km', current, current, precision=lax.Precision.HIGHEST) / ROWS
    factor = jnp.linalg.cholesky(gram)
    flat = current.transpose(1, 0, 2).reshape(VECTORS, ROWS)
    basis = jax.scipy.linalg.solve_triangular(factor, flat, lower=True)
    return (basis, factor)
```

```python
import functools
import math

import jax
import jax.numpy as jnp
from jax import lax
from jax.experimental import pallas as pl
from jax.experimental.pallas import tpu as pltpu
from jax.sharding import PartitionSpec as P

AXES = ("gx", "gy")
BAND = 128
MOST = 2
DEGREE = 4
GROUP = 8
STEP_BANDS = 4

LOW_EDGE = 0.2
HIGH_EDGE = 2.0

VMEM = pltpu.VMEM
SMEM = pltpu.SMEM


def chebyshev_terms():
    centre = 0.5 * (LOW_EDGE + HIGH_EDGE)
    halfwidth = 0.5 * (HIGH_EDGE - LOW_EDGE)
    anchor = -centre / halfwidth
    values = [1.0, anchor]
    for repeat in range(DEGREE - 1):
        values.append(2.0 * anchor * values[-1] - values[-2])
    return (centre, halfwidth, values)


def exchange(blocks):
    return lax.all_to_all(blocks, AXES, split_axis=0, concat_axis=0, tiled=True)


def whole(space=VMEM):
    return pl.BlockSpec(memory_space=space)


def tile_groups(work, count, rows, coords, wcol, pcol, rvec, tiles, deg, stage, sems):
    groups = (count[0] + GROUP - 1) // GROUP

    def copies(group, slot):
        return [
            pltpu.make_async_copy(
                stage.at[slot, u], tiles.at[work[0, group * GROUP + u]], sems.at[slot, u]
            )
            for u in range(GROUP)
        ]

    def body(group, carry):
        slot = lax.rem(group, 2)

        @pl.when(group >= 2)
        def _():
            for copy in copies(group - 2, slot):
                copy.wait()

        for u in range(GROUP):
            at = group * GROUP + u
            band = work[1, at]
            entry = work[2, at]
            keep = work[3, at].astype(jnp.float32)
            inner = lax.dot_general(
                coords[entry], rows[band], (((1,), (1,)), ((), ())),
                preferred_element_type=jnp.float32,
            )
            half_sq = rvec[band, 0:1, :]
            row_width = rvec[band, 1:2, :]
            power = ((inner - half_sq) * wcol[entry] - pcol[entry]) * row_width
            weights = jnp.exp2(power) * keep
            stage[slot, u] = weights.astype(jnp.bfloat16)
            deg[band] += jnp.sum(weights.reshape(BAND // 8, 8, BAND), axis=0)
        for copy in copies(group, slot):
            copy.start()
        return carry

    lax.fori_loop(0, groups, body, 0)
    for back in (2, 1):
        @pl.when(groups >= back)
        def _():
            group = groups - back
            for copy in copies(group, lax.rem(group, 2)):
                copy.wait()


def local_kernel(work, count, rows, wcol, pcol, rvec, tiles, deg, stage, sems):
    deg[...] = jnp.zeros(deg.shape, deg.dtype)
    tile_groups(work, count, rows, rows, wcol, pcol, rvec, tiles, deg, stage, sems)


def pack_rows(send_index, scaled, send):
    def one(at, carry):
        send[at] = scaled[send_index[at]]
        return carry

    lax.fori_loop(0, send.shape[0], one, 0, unroll=8)


def remote_kernel(work, count, send_index, rows, coords, wcol, pcol, rvec, deg_in, start, tiles_in,
                  tiles, root, scaled, send, deg, stage, sems):
    deg[...] = deg_in[...]
    tile_groups(work, count, rows, coords, wcol, pcol, rvec, tiles, deg, stage, sems)
    for band in range(deg.shape[0]):
        total = jnp.sum(deg[band], axis=0, keepdims=True)
        inverse = 1.0 / jnp.sqrt(total)
        root[band : band + 1, :] = inverse
        block = start[:, band * BAND : (band + 1) * BAND]
        scaled[band] = (block * inverse).astype(jnp.bfloat16)
    pack_rows(send_index, scaled, send)


def round_kernel(first, last, gains, slots, send_index, slot_pos, scaled_in, got, tiles, root, cur, prev,
                 following, *rest):
    if last:
        gram, table = rest
    else:
        scaled, send, table = rest
    step = pl.program_id(0)
    bands = scaled_in.shape[0]

    @pl.when(step == 0)
    def _():
        table[0:bands] = scaled_in[...]
        table[bands:] = got[...]
        if last:
            gram[...] = jnp.zeros(gram.shape, gram.dtype)

    own, mixed_gain, old = gains
    for sub in range(STEP_BANDS):
        band = step * STEP_BANDS + sub
        lhs = jnp.concatenate([table[slot_pos[band * slots + j]] for j in range(slots)], axis=1)
        rhs = tiles[sub * slots : (sub + 1) * slots].reshape(slots * BAND, BAND)
        mixed = jnp.dot(lhs, rhs, preferred_element_type=jnp.float32)
        inverse = root[pl.ds(band, 1), :]
        lanes = slice(sub * BAND, (sub + 1) * BAND)
        block = own * cur[:, lanes] + (mixed_gain * inverse) * mixed
        if not first:
            block = block - old * prev[:, lanes]
        following[:, lanes] = block
        if not last:
            scaled[band] = (inverse * block).astype(jnp.bfloat16)
    if last:
        piece = following[...]
        gram[...] += lax.dot_general(
            piece, piece, (((1,), (1,)), ((), ())),
            precision=lax.Precision.HIGHEST, preferred_element_type=jnp.float32,
        )
    else:
        @pl.when(step == pl.num_programs(0) - 1)
        def _():
            pack_rows(send_index, scaled, send)


def finish_kernel(total_rows, parts, flat, basis, factor):
    vectors = flat.shape[0]
    gram = jnp.sum(parts[...], axis=0) / total_rows
    row_ids = lax.broadcasted_iota(jnp.int32, (vectors, vectors), 0)
    col_ids = lax.broadcasted_iota(jnp.int32, (vectors, vectors), 1)
    left = gram
    right = jnp.where(row_ids == col_ids, 1.0, 0.0).astype(jnp.float32)
    lower = jnp.zeros((vectors, vectors), jnp.float32)
    scale = jnp.zeros((vectors, 1), jnp.float32)
    rows = lax.broadcasted_iota(jnp.int32, (vectors, 1), 0)
    for j in range(vectors):
        pivot = left[j : j + 1, j : j + 1]
        inverse = 1.0 / pivot
        column = left[:, j : j + 1]
        ratio = jnp.where(rows > j, column * inverse, 0.0)
        spread = lax.rsqrt(pivot)
        spread = 1.0 / jnp.sqrt(pivot)
        scale = jnp.where(rows == j, spread, scale)
        lower = jnp.where((col_ids == j) & (row_ids >= j), column * spread, lower)
        left_row = left[j : j + 1, :]
        right_row = right[j : j + 1, :]
        left = left - ratio * left_row
        right = right - ratio * right_row
    factor[...] = lower
    basis[...] = jnp.dot(
        right * scale, flat[...], precision=lax.Precision.HIGHEST, preferred_element_type=jnp.float32
    )


def on_device(features, inv_width, start_block, neighbour_ids, slot_mask):
    bands, slots = neighbour_ids.shape
    dims = features.shape[1]
    vectors = start_block.shape[0]
    devices = lax.axis_size(AXES)
    device = lax.axis_index(AXES)
    entries = devices * MOST
    count_all = bands * slots
    listed = count_all + GROUP

    owner_dev = neighbour_ids // bands
    within = neighbour_ids % bands
    remote = (slot_mask == 1) & (owner_dev != device)
    flat_remote = remote.reshape(-1)
    all_bands = jnp.arange(devices * bands, dtype=jnp.int32)
    matches = (neighbour_ids.reshape(-1)[:, None] == all_bands[None, :]) & flat_remote[:, None]
    need_mine = jnp.any(matches, axis=0).astype(jnp.int32).reshape(devices, bands)
    wanted = exchange(need_mine)
    rank_send = jnp.cumsum(wanted, axis=1) - 1
    picks = (wanted[:, None, :] == 1) & (
        rank_send[:, None, :] == jnp.arange(MOST, dtype=jnp.int32)[None, :, None]
    )
    send_index = jnp.sum(
        picks.astype(jnp.int32) * jnp.arange(bands, dtype=jnp.int32)[None, None, :], axis=2
    ).reshape(-1)

    feature_bands = features.reshape(bands, BAND, dims)
    widths = inv_width.reshape(bands, BAND).astype(jnp.float32)
    squares = jnp.sum(jnp.square(feature_bands.astype(jnp.float32)), axis=2)
    sides = jnp.stack([widths, 0.5 * squares * widths], axis=1)
    got_sides = exchange(
        jnp.take(sides, send_index, axis=0, mode="clip").reshape(devices, MOST * 2, BAND)
    ).reshape(entries, 2, BAND)
    send_coords = jnp.take(feature_bands, send_index, axis=0, mode="clip")
    got_coords = exchange(send_coords.reshape(devices, MOST, BAND, dims)).reshape(entries, BAND, dims)

    rank_mine = jnp.cumsum(need_mine, axis=1) - 1
    rank_lookup = jnp.take(rank_mine.reshape(-1), neighbour_ids, axis=0, mode="clip")
    got_pos = owner_dev * MOST + rank_lookup
    slot_pos = jnp.where(remote, bands + got_pos, within).reshape(-1)
    entry_of = jnp.where(remote, got_pos, within).reshape(-1)
    mask_of = slot_mask.reshape(-1)

    where_at = jnp.arange(listed, dtype=jnp.int32)
    order = jnp.arange(count_all, dtype=jnp.int32)

    def work_list(chosen):
        count = jnp.sum(chosen.astype(jnp.int32))
        place = jnp.cumsum(chosen.astype(jnp.int32)) - 1
        hit = ((place[None, :] == where_at[:, None]) & chosen[None, :]).astype(jnp.int32)
        tile_id = jnp.sum(hit * order[None, :], axis=1)
        entry = jnp.sum(hit * entry_of[None, :], axis=1)
        keep = jnp.sum(hit * mask_of[None, :], axis=1)
        used = where_at < count
        target = jnp.where(used, tile_id, count_all + where_at % GROUP)
        return jnp.stack([target, tile_id // slots, entry, keep]), count.reshape(1)

    local_work, local_count = work_list(~flat_remote)
    remote_work, remote_count = work_list(flat_remote)

    rvec = jnp.stack([0.5 * squares, (2.0 * math.log2(math.e)) * widths], axis=1)

    def columns(rows):
        return jnp.broadcast_to(rows[:, :, None], rows.shape + (BAND,))

    tile_shape = jax.ShapeDtypeStruct((count_all + GROUP, BAND, BAND), jnp.bfloat16)
    stage = [
        pltpu.VMEM((2, GROUP, BAND, BAND), jnp.bfloat16),
        pltpu.SemaphoreType.DMA((2, GROUP)),
    ]
    build_flops = 2 * count_all * BAND * BAND * dims
    tiles, deg = pl.pallas_call(
        local_kernel,
        out_shape=(tile_shape, jax.ShapeDtypeStruct((bands, 8, BAND), jnp.float32)),
        in_specs=[whole(SMEM)] * 2 + [whole()] * 4,
        out_specs=(whole(pl.ANY), whole()),
        scratch_shapes=stage,
        cost_estimate=pl.CostEstimate(
            flops=build_flops, bytes_accessed=2 * count_all * BAND * BAND, transcendentals=count_all * BAND * BAND
        ),
        name="local_tiles",
    )(local_work, local_count, feature_bands, columns(sides[:, 0]), columns(sides[:, 1]), rvec)

    row_shape = jax.ShapeDtypeStruct((bands, vectors, BAND), jnp.bfloat16)
    send_shape = jax.ShapeDtypeStruct((entries, vectors, BAND), jnp.bfloat16)
    tiles, root, scaled, send = pl.pallas_call(
        remote_kernel,
        out_shape=(tile_shape, jax.ShapeDtypeStruct((bands, BAND), jnp.float32), row_shape, send_shape),
        in_specs=[whole(SMEM)] * 3 + [whole()] * 7 + [whole(pl.ANY)],
        out_specs=(whole(pl.ANY), whole(), whole(), whole()),
        scratch_shapes=[pltpu.VMEM((bands, 8, BAND), jnp.float32)] + stage,
        input_output_aliases={10: 0},
        cost_estimate=pl.CostEstimate(
            flops=build_flops // 2, bytes_accessed=count_all * BAND * BAND, transcendentals=count_all * BAND * BAND
        ),
        name="remote_tiles",
    )(remote_work, remote_count, send_index, feature_bands, got_coords, columns(got_sides[:, 0]),
      columns(got_sides[:, 1]), rvec, deg, start_block, tiles)

    centre, halfwidth, values = chebyshev_terms()
    flat_shape = jax.ShapeDtypeStruct((vectors, bands * BAND), jnp.float32)
    flat_spec = pl.BlockSpec((vectors, STEP_BANDS * BAND), lambda i: (0, i))
    fixed3 = lambda i: (0, 0, 0)
    previous, current = start_block, start_block
    for power in range(DEGREE):
        first, last = power == 0, power == DEGREE - 1
        if first:
            lead, old = 1.0 / values[1], 0.0
        else:
            lead = 2.0 * values[power] / values[power + 1]
            old = values[power - 1] / values[power + 1]
        gains = (lead * (1.0 - centre) / halfwidth, -lead / halfwidth, old)
        got = exchange(send.reshape(devices, MOST, vectors, BAND)).reshape(entries, vectors, BAND)
        if last:
            outs = (flat_shape, jax.ShapeDtypeStruct((vectors, vectors), jnp.float32))
            out_specs = (flat_spec, pl.BlockSpec((vectors, vectors), lambda i: (0, 0)))
        else:
            outs = (flat_shape, row_shape, send_shape)
            out_specs = (
                flat_spec,
                pl.BlockSpec(row_shape.shape, fixed3),
                pl.BlockSpec(send_shape.shape, fixed3),
            )
        results = pl.pallas_call(
            functools.partial(round_kernel, first, last, gains, slots),
            grid=(bands // STEP_BANDS,),
            out_shape=outs,
            in_specs=[
                whole(SMEM),
                whole(SMEM),
                pl.BlockSpec(row_shape.shape, fixed3),
                pl.BlockSpec(send_shape.shape, fixed3),
                pl.BlockSpec((STEP_BANDS * slots, BAND, BAND), lambda i: (i, 0, 0)),
                pl.BlockSpec((bands, BAND), lambda i: (0, 0)),
                flat_spec,
                flat_spec,
            ],
            out_specs=out_specs,
            scratch_shapes=[pltpu.VMEM((bands + entries, vectors, BAND), jnp.bfloat16)],
            cost_estimate=pl.CostEstimate(
                flops=2 * count_all * BAND * BAND * vectors,
                bytes_accessed=2 * count_all * BAND * BAND,
                transcendentals=0,
            ),
            name="round" + str(power),
        )(send_index, slot_pos, scaled, got, tiles, root, current, previous)
        previous, current = current, results[0]
        if last:
            partial_gram = results[1]
        else:
            scaled, send = results[1], results[2]

    parts = exchange(jnp.broadcast_to(partial_gram[None], (devices, vectors, vectors)))
    basis, factor = pl.pallas_call(
        functools.partial(finish_kernel, devices * bands * BAND),
        out_shape=(flat_shape, jax.ShapeDtypeStruct((vectors, vectors), jnp.float32)),
        in_specs=[whole()] * 2,
        out_specs=(whole(), whole()),
        name="finish",
    )(parts, current)
    return (basis, factor)


def solution(mesh):
    placed = (P(AXES, None), P(AXES), P(None, AXES), P(AXES, None), P(AXES, None))
    return jax.shard_map(
        on_device,
        mesh=mesh,
        in_specs=placed,
        out_specs=(P(None, AXES), P()),
        check_vma=False,
    )
```

```python
import functools
import math

import jax
import jax.numpy as jnp
from jax import lax
from jax.experimental import pallas as pl
from jax.experimental.pallas import tpu as pltpu
from jax.sharding import PartitionSpec as P

AXES = ("gx", "gy")
BAND = 128
MOST = 2
DEGREE = 4
GROUP = 16
STAGES = 4
EXTRA = 8

LOW_EDGE = 0.2
HIGH_EDGE = 2.0

VMEM = pltpu.VMEM
SMEM = pltpu.SMEM


def chebyshev_terms():
    centre = 0.5 * (LOW_EDGE + HIGH_EDGE)
    halfwidth = 0.5 * (HIGH_EDGE - LOW_EDGE)
    anchor = -centre / halfwidth
    values = [1.0, anchor]
    for repeat in range(DEGREE - 1):
        values.append(2.0 * anchor * values[-1] - values[-2])
    return (centre, halfwidth, values)


def exchange(blocks):
    return lax.all_to_all(blocks, AXES, split_axis=0, concat_axis=0, tiled=True)


def whole(space=VMEM):
    return pl.BlockSpec(memory_space=space)


def need_kernel(ids, mask, need):
    slots, bands = ids.shape
    devices = need.shape[0]
    device_ids = lax.broadcasted_iota(jnp.int32, (devices, bands), 0)
    band_ids = lax.broadcasted_iota(jnp.int32, (bands, bands), 0)
    owners, withins = [], []
    for j in range(slots):
        row = ids[j : j + 1, :]
        keep = mask[j : j + 1, :] == 1
        owners.append(jnp.where((row // bands == device_ids) & keep, 1.0, 0.0))
        withins.append(jnp.where(row % bands == band_ids, 1.0, 0.0))
    count = lax.dot_general(
        jnp.concatenate(owners, axis=1).astype(jnp.bfloat16),
        jnp.concatenate(withins, axis=1).astype(jnp.bfloat16),
        (((1,), (1,)), ((), ())),
        preferred_element_type=jnp.float32,
    )
    need[...] = jnp.where(count > 0.0, 1, 0).astype(jnp.int32)


def pack_kernel(send_index, features, sides, send, tails, sems):
    devices = send.shape[0]

    def bands_of(d):
        return [
            pltpu.make_async_copy(
                features.at[send_index[d * MOST + h]],
                send.at[d, pl.ds(h * BAND, BAND)],
                sems.at[h, d],
            )
            for h in range(MOST)
        ]

    def tail_of(d):
        return pltpu.make_async_copy(
            tails.at[d], send.at[d, pl.ds(MOST * BAND, EXTRA)], sems.at[MOST, d]
        )

    def first(d, carry):
        for copy in bands_of(d):
            copy.start()
        tails[d] = jnp.concatenate([sides[send_index[d * MOST + h]] for h in range(MOST)], axis=1)
        return carry

    def second(d, carry):
        tail_of(d).start()
        return carry

    def third(d, carry):
        for copy in bands_of(d):
            copy.wait()
        tail_of(d).wait()
        return carry

    lax.fori_loop(0, devices, first, 0)
    lax.fori_loop(0, devices, second, 0)
    lax.fori_loop(0, devices, third, 0)


def spread_column(side):
    row = lax.broadcasted_iota(jnp.int32, (EXTRA, 2 * BAND), 0)
    lane = lax.broadcasted_iota(jnp.int32, (EXTRA, 2 * BAND), 1)
    left = jnp.where((row == 0) & (lane < BAND), 1.0, 0.0)
    right = jnp.where((row > 0) & (row < 4) & (lane >= BAND), 1.0, 0.0)
    return lax.dot_general(
        side, (left + right).astype(jnp.bfloat16), (((0,), (0,)), ((), ())),
        preferred_element_type=jnp.float32,
    )


def tile_groups(work, count, rows, coords_of, cols, rvec, tiles, deg, stage, sems):
    groups = (count[0] + GROUP - 1) // GROUP

    def copy_of(group):
        slot = lax.rem(group, STAGES)
        return pltpu.make_async_copy(
            stage.at[slot], tiles.at[pl.ds(group * GROUP, GROUP)], sems.at[slot]
        )

    def body(group, carry):
        slot = lax.rem(group, STAGES)

        @pl.when(group >= STAGES)
        def _():
            copy_of(group - STAGES).wait()

        for u in range(GROUP):
            at = group * GROUP + u
            band = work[0, at]
            entry = work[1, at]
            keep = work[2, at].astype(jnp.float32)
            inner = lax.dot_general(
                coords_of(entry), rows[band], (((1,), (1,)), ((), ())),
                preferred_element_type=jnp.float32,
            )
            half_sq = rvec[band, 0:1, :]
            row_width = rvec[band, 1:2, :]
            power = ((inner - half_sq) * cols[entry, :, 0:BAND] - cols[entry, :, BAND:]) * row_width
            weights = jnp.exp2(power) * keep
            stage[slot, u] = weights.astype(jnp.bfloat16)
            deg[band] += jnp.sum(weights.reshape(BAND // 8, 8, BAND), axis=0)
        copy_of(group).start()
        return carry

    lax.fori_loop(0, groups, body, 0)
    for back in range(STAGES, 0, -1):
        @pl.when(groups >= back)
        def _():
            copy_of(groups - back).wait()


def local_kernel(work, count, rows, sides, rvec, tiles, deg, cols, stage, sems):
    deg[...] = jnp.zeros(deg.shape, deg.dtype)

    def fill(band, carry):
        cols[band] = spread_column(sides[band])
        return carry

    lax.fori_loop(0, rows.shape[0], fill, 0, unroll=4)
    tile_groups(work, count, rows, lambda entry: rows[entry], cols, rvec, tiles, deg, stage, sems)


def pack_rows(send_index, scaled, send):
    def one(at, carry):
        send[at] = scaled[send_index[at]]
        return carry

    lax.fori_loop(0, send.shape[0], one, 0, unroll=8)


def remote_kernel(work, count, send_index, rows, got, rvec, deg_in, start,
                  tiles, root, scaled, send, deg, cols, stage, sems):
    deg[...] = deg_in[...]
    tail = MOST * BAND

    def fill(owner, carry):
        for h in range(MOST):
            side = got[owner, tail : tail + EXTRA, h * BAND : (h + 1) * BAND]
            cols[owner * MOST + h] = spread_column(side)
        return carry

    lax.fori_loop(0, got.shape[0], fill, 0, unroll=4)

    def coords_of(entry):
        at = pl.multiple_of(lax.rem(entry, MOST) * BAND, BAND)
        return got[entry // MOST, pl.ds(at, BAND), :]

    tile_groups(work, count, rows, coords_of, cols, rvec, tiles, deg, stage, sems)
    for band in range(deg.shape[0]):
        total = jnp.sum(deg[band], axis=0, keepdims=True)
        inverse = 1.0 / jnp.sqrt(total)
        root[band : band + 1, :] = inverse
        block = start[:, band * BAND : (band + 1) * BAND]
        scaled[band] = (block * inverse).astype(jnp.bfloat16)
    pack_rows(send_index, scaled, send)


def gather_product(work, count, table, tiles, total, held, sems):
    groups = (count[0] + GROUP - 1) // GROUP

    def copy_of(group):
        part = pl.ds(group * GROUP, GROUP)
        return pltpu.make_async_copy(tiles.at[part], held.at[part], sems.at[group])

    def begin(group, carry):
        copy_of(group).start()
        return carry

    def body(group, carry):
        copy_of(group).wait()
        for u in range(GROUP):
            at = group * GROUP + u
            total[work[0, at]] += jnp.dot(
                table[work[1, at]], held[at], preferred_element_type=jnp.float32
            )
        return carry

    lax.fori_loop(0, groups, begin, 0)
    lax.fori_loop(0, groups, body, 0)


def own_kernel(work, count, scaled, tiles, total, held, sems):
    total[...] = jnp.zeros(total.shape, total.dtype)
    gather_product(work, count, scaled, tiles, total, held, sems)


def fold(square):
    return jnp.concatenate([square[8 * q : 8 * q + 8, :] for q in range(square.shape[0] // 8)], axis=1)


def unfold(packed, side):
    return jnp.concatenate([packed[:, side * q : side * (q + 1)] for q in range(side // 8)], axis=0)


def round_kernel(first, last, gains, work, count, send_index, got, total_in, root, cur, prev, tiles,
                 following, *rest):
    if last:
        gram, total, held, sems = rest
    else:
        scaled, send, total, held, sems = rest
    total[...] = total_in[...]
    gather_product(work, count, got, tiles, total, held, sems)
    own, mixed_gain, old = gains
    for band in range(total.shape[0]):
        inverse = root[band : band + 1, :]
        lanes = slice(band * BAND, (band + 1) * BAND)
        block = own * cur[:, lanes] + (mixed_gain * inverse) * total[band]
        if not first:
            block = block - old * prev[:, lanes]
        following[:, lanes] = block
        if not last:
            scaled[band] = (inverse * block).astype(jnp.bfloat16)
    if last:
        piece = following[...]
        square = lax.dot_general(
            piece, piece, (((1,), (1,)), ((), ())),
            precision=lax.Precision.HIGHEST, preferred_element_type=jnp.float32,
        )
        gram[...] = jnp.broadcast_to(fold(square)[None], gram.shape)
    else:
        pack_rows(send_index, scaled, send)


def finish_kernel(total_rows, parts, flat, basis, factor):
    vectors = flat.shape[0]
    gram = unfold(jnp.sum(parts[...], axis=0), vectors) / total_rows
    row_ids = lax.broadcasted_iota(jnp.int32, (vectors, vectors), 0)
    col_ids = lax.broadcasted_iota(jnp.int32, (vectors, vectors), 1)
    left = gram
    right = jnp.where(row_ids == col_ids, 1.0, 0.0).astype(jnp.float32)
    lower = jnp.zeros((vectors, vectors), jnp.float32)
    scale = jnp.zeros((vectors, 1), jnp.float32)
    rows = lax.broadcasted_iota(jnp.int32, (vectors, 1), 0)
    for j in range(vectors):
        pivot = left[j : j + 1, j : j + 1]
        inverse = 1.0 / pivot
        column = left[:, j : j + 1]
        ratio = jnp.where(rows > j, column * inverse, 0.0)
        spread = 1.0 / jnp.sqrt(pivot)
        scale = jnp.where(rows == j, spread, scale)
        lower = jnp.where((col_ids == j) & (row_ids >= j), column * spread, lower)
        left_row = left[j : j + 1, :]
        right_row = right[j : j + 1, :]
        left = left - ratio * left_row
        right = right - ratio * right_row
    factor[...] = lower
    basis[...] = jnp.dot(
        right * scale, flat[...], precision=lax.Precision.HIGHEST, preferred_element_type=jnp.float32
    )


def on_device(features, inv_width, start_block, neighbour_ids, slot_mask):
    bands, slots = neighbour_ids.shape
    dims = features.shape[1]
    vectors = start_block.shape[0]
    devices = lax.axis_size(AXES)
    device = lax.axis_index(AXES)
    entries = devices * MOST
    count_all = bands * slots

    ids = neighbour_ids.T
    mask = slot_mask.T
    need_mine = pl.pallas_call(
        need_kernel,
        out_shape=jax.ShapeDtypeStruct((devices, bands), jnp.int32),
        in_specs=[whole()] * 2,
        out_specs=whole(),
        name="need",
    )(ids, mask)
    wanted = exchange(need_mine)
    rank_send = jnp.cumsum(wanted, axis=1) - 1
    picks = (wanted[:, None, :] == 1) & (
        rank_send[:, None, :] == jnp.arange(MOST, dtype=jnp.int32)[None, :, None]
    )
    send_index = jnp.sum(
        picks.astype(jnp.int32) * jnp.arange(bands, dtype=jnp.int32)[None, None, :], axis=2
    ).reshape(-1)

    feature_bands = features.reshape(bands, BAND, dims)
    widths = inv_width.reshape(bands, BAND).astype(jnp.float32)
    squares = jnp.sum(jnp.square(feature_bands.astype(jnp.float32)), axis=2)
    product = 0.5 * squares * widths
    high = lax.reduce_precision(product, 8, 7)
    rest = product - high
    middle = lax.reduce_precision(rest, 8, 7)
    blank = jnp.zeros_like(widths)
    sides = jnp.stack(
        [widths, high, middle, rest - middle] + [blank] * (EXTRA - 4), axis=1
    ).astype(jnp.bfloat16)
    send_coords = pl.pallas_call(
        pack_kernel,
        out_shape=jax.ShapeDtypeStruct((devices, MOST * BAND + EXTRA, dims), jnp.bfloat16),
        in_specs=[whole(SMEM)] + [whole()] * 2,
        out_specs=whole(pl.ANY),
        scratch_shapes=[
            pltpu.VMEM((devices, EXTRA, dims), jnp.bfloat16),
            pltpu.SemaphoreType.DMA((MOST + 1, devices)),
        ],
        name="pack",
    )(send_index, feature_bands, sides)
    got_coords = exchange(send_coords)

    flat_ids = ids.reshape(-1)
    active = mask.reshape(-1) == 1
    owner_dev = flat_ids // bands
    within = flat_ids % bands
    far = active & (owner_dev != device)
    rank_mine = jnp.cumsum(need_mine, axis=1) - 1
    rank_lookup = jnp.take(rank_mine.reshape(-1), flat_ids, axis=0, mode="clip")
    entry_of = jnp.where(far, owner_dev * MOST + rank_lookup, within)
    order = jnp.arange(count_all, dtype=jnp.int32)

    def work_list(chosen):
        ones = chosen.astype(jnp.int32)
        place = jnp.cumsum(ones) - 1
        hit = ((place[None, :] == order[:, None]) & chosen[None, :]).astype(jnp.int32)
        tile_id = jnp.sum(hit * order[None, :], axis=1)
        entry = jnp.sum(hit * entry_of[None, :], axis=1)
        count = jnp.sum(ones)
        keep = (order < count).astype(jnp.int32)
        return jnp.stack([tile_id % bands, entry, keep]), count.reshape(1)

    near_work, near_count = work_list(active & ~far)
    far_work, far_count = work_list(far)

    rvec = jnp.stack([0.5 * squares, (2.0 * math.log2(math.e)) * widths], axis=1)

    tile_shape = jax.ShapeDtypeStruct((count_all, BAND, BAND), jnp.bfloat16)

    def building(columns):
        return [
            pltpu.VMEM((columns, BAND, 2 * BAND), jnp.float32),
            pltpu.VMEM((STAGES, GROUP, BAND, BAND), jnp.bfloat16),
            pltpu.SemaphoreType.DMA((STAGES,)),
        ]

    tile_area = count_all * BAND * BAND
    build_cost = pl.CostEstimate(
        flops=tile_area * dims, bytes_accessed=tile_area, transcendentals=tile_area // 2
    )
    near_tiles, deg = pl.pallas_call(
        local_kernel,
        out_shape=(tile_shape, jax.ShapeDtypeStruct((bands, 8, BAND), jnp.float32)),
        in_specs=[whole(SMEM)] * 2 + [whole()] * 3,
        out_specs=(whole(pl.ANY), whole()),
        scratch_shapes=building(bands),
        cost_estimate=build_cost,
        name="local_tiles",
    )(near_work, near_count, feature_bands, sides, rvec)

    row_shape = jax.ShapeDtypeStruct((bands, vectors, BAND), jnp.bfloat16)
    send_shape = jax.ShapeDtypeStruct((entries, vectors, BAND), jnp.bfloat16)
    far_tiles, root, scaled, send = pl.pallas_call(
        remote_kernel,
        out_shape=(tile_shape, jax.ShapeDtypeStruct((bands, BAND), jnp.float32), row_shape, send_shape),
        in_specs=[whole(SMEM)] * 3 + [whole()] * 5,
        out_specs=(whole(pl.ANY), whole(), whole(), whole()),
        scratch_shapes=[pltpu.VMEM((bands, 8, BAND), jnp.float32)] + building(entries),
        cost_estimate=build_cost,
        name="remote_tiles",
    )(far_work, far_count, send_index, feature_bands, got_coords, rvec, deg, start_block)

    centre, halfwidth, values = chebyshev_terms()
    flat_shape = jax.ShapeDtypeStruct((vectors, bands * BAND), jnp.float32)
    total_shape = jax.ShapeDtypeStruct((bands, vectors, BAND), jnp.float32)
    gram_shape = jax.ShapeDtypeStruct((devices, 8, vectors * vectors // 8), jnp.float32)
    fetching = [
        pltpu.VMEM((count_all, BAND, BAND), jnp.bfloat16),
        pltpu.SemaphoreType.DMA((count_all // GROUP,)),
    ]
    product_cost = pl.CostEstimate(
        flops=tile_area * vectors, bytes_accessed=tile_area, transcendentals=0
    )
    previous, current = start_block, start_block
    for power in range(DEGREE):
        first, last = power == 0, power == DEGREE - 1
        if first:
            lead, old = 1.0 / values[1], 0.0
        else:
            lead = 2.0 * values[power] / values[power + 1]
            old = values[power - 1] / values[power + 1]
        gains = (lead * (1.0 - centre) / halfwidth, -lead / halfwidth, old)
        got = exchange(send.reshape(devices, MOST, vectors, BAND)).reshape(entries, vectors, BAND)
        own_total = pl.pallas_call(
            own_kernel,
            out_shape=total_shape,
            in_specs=[whole(SMEM)] * 2 + [whole(), whole(pl.ANY)],
            out_specs=whole(),
            scratch_shapes=fetching,
            cost_estimate=product_cost,
            name="own" + str(power),
        )(near_work, near_count, scaled, near_tiles)
        outs = (flat_shape, gram_shape) if last else (flat_shape, row_shape, send_shape)
        results = pl.pallas_call(
            functools.partial(round_kernel, first, last, gains),
            out_shape=outs,
            in_specs=[whole(SMEM)] * 3 + [whole()] * 5 + [whole(pl.ANY)],
            out_specs=tuple([whole()] * len(outs)),
            scratch_shapes=[pltpu.VMEM((bands, vectors, BAND), jnp.float32)] + fetching,
            cost_estimate=product_cost,
            name="round" + str(power),
        )(far_work, far_count, send_index, got, own_total, root, current, previous, far_tiles)
        previous, current = current, results[0]
        if last:
            parts = exchange(results[1])
        else:
            scaled, send = results[1], results[2]

    basis, factor = pl.pallas_call(
        functools.partial(finish_kernel, devices * bands * BAND),
        out_shape=(flat_shape, jax.ShapeDtypeStruct((vectors, vectors), jnp.float32)),
        in_specs=[whole()] * 2,
        out_specs=(whole(), whole()),
        name="finish",
    )(parts, current)
    return (basis, factor)


def solution(mesh):
    placed = (P(AXES, None), P(AXES), P(None, AXES), P(AXES, None), P(AXES, None))
    return jax.shard_map(
        on_device,
        mesh=mesh,
        in_specs=placed,
        out_specs=(P(None, AXES), P()),
        check_vma=False,
    )
```

```python
import functools
import math

import jax
import jax.numpy as jnp
from jax import lax
from jax.experimental import pallas as pl
from jax.experimental.pallas import tpu as pltpu
from jax.sharding import PartitionSpec as P

AXES = ("gx", "gy")
BAND = 128
MOST = 2
DEGREE = 4
GROUP = 16
STAGES = 4
EXTRA = 8
LIMIT = 50 * 1024 * 1024

LOW_EDGE = 0.2
HIGH_EDGE = 2.0

VMEM = pltpu.VMEM
SMEM = pltpu.SMEM


def chebyshev_terms():
    centre = 0.5 * (LOW_EDGE + HIGH_EDGE)
    halfwidth = 0.5 * (HIGH_EDGE - LOW_EDGE)
    anchor = -centre / halfwidth
    values = [1.0, anchor]
    for repeat in range(DEGREE - 1):
        values.append(2.0 * anchor * values[-1] - values[-2])
    return (centre, halfwidth, values)


def exchange(blocks):
    return lax.all_to_all(blocks, AXES, split_axis=0, concat_axis=0, tiled=True)


def whole(space=VMEM):
    return pl.BlockSpec(memory_space=space)


def need_kernel(ids, mask, need):
    slots, bands = ids.shape
    devices = need.shape[0]
    device_ids = lax.broadcasted_iota(jnp.int32, (devices, bands), 0)
    band_ids = lax.broadcasted_iota(jnp.int32, (bands, bands), 0)
    owners, withins = [], []
    for j in range(slots):
        row = ids[j : j + 1, :]
        keep = mask[j : j + 1, :] == 1
        owners.append(jnp.where((row // bands == device_ids) & keep, 1.0, 0.0))
        withins.append(jnp.where(row % bands == band_ids, 1.0, 0.0))
    count = lax.dot_general(
        jnp.concatenate(owners, axis=1).astype(jnp.bfloat16),
        jnp.concatenate(withins, axis=1).astype(jnp.bfloat16),
        (((1,), (1,)), ((), ())),
        preferred_element_type=jnp.float32,
    )
    need[...] = jnp.where(count > 0.0, 1, 0).astype(jnp.int32)


def pack_kernel(send_index, features, sides, send, tails, sems):
    devices = send.shape[0]

    def bands_of(d):
        return [
            pltpu.make_async_copy(
                features.at[send_index[d * MOST + h]],
                send.at[d, pl.ds(h * BAND, BAND)],
                sems.at[h, d],
            )
            for h in range(MOST)
        ]

    def tail_of(d):
        return pltpu.make_async_copy(
            tails.at[d], send.at[d, pl.ds(MOST * BAND, EXTRA)], sems.at[MOST, d]
        )

    def first(d, carry):
        for copy in bands_of(d):
            copy.start()
        tails[d] = jnp.concatenate([sides[send_index[d * MOST + h]] for h in range(MOST)], axis=1)
        return carry

    def second(d, carry):
        tail_of(d).start()
        return carry

    def third(d, carry):
        for copy in bands_of(d):
            copy.wait()
        tail_of(d).wait()
        return carry

    lax.fori_loop(0, devices, first, 0)
    lax.fori_loop(0, devices, second, 0)
    lax.fori_loop(0, devices, third, 0)


def spread_column(side):
    row = lax.broadcasted_iota(jnp.int32, (EXTRA, 2 * BAND), 0)
    lane = lax.broadcasted_iota(jnp.int32, (EXTRA, 2 * BAND), 1)
    left = jnp.where((row == 0) & (lane < BAND), 1.0, 0.0)
    right = jnp.where((row > 0) & (row < 4) & (lane >= BAND), 1.0, 0.0)
    return lax.dot_general(
        side, (left + right).astype(jnp.bfloat16), (((0,), (0,)), ((), ())),
        preferred_element_type=jnp.float32,
    )


def tile_groups(work, count, rows, coords_of, cols, rvec, tiles, deg, stage, sems):
    groups = (count[0] + GROUP - 1) // GROUP

    def copy_of(group):
        slot = lax.rem(group, STAGES)
        return pltpu.make_async_copy(
            stage.at[slot], tiles.at[pl.ds(group * GROUP, GROUP)], sems.at[slot]
        )

    def body(group, carry):
        slot = lax.rem(group, STAGES)

        @pl.when(group >= STAGES)
        def _():
            copy_of(group - STAGES).wait()

        for u in range(GROUP):
            at = group * GROUP + u
            band = work[0, at]
            entry = work[1, at]
            keep = work[2, at].astype(jnp.float32)
            inner = lax.dot_general(
                coords_of(entry), rows[band], (((1,), (1,)), ((), ())),
                preferred_element_type=jnp.float32,
            )
            half_sq = rvec[band, 0:1, :]
            row_width = rvec[band, 1:2, :]
            power = ((inner - half_sq) * cols[entry, :, 0:BAND] - cols[entry, :, BAND:]) * row_width
            weights = jnp.exp2(power) * keep
            stage[slot, u] = weights.astype(jnp.bfloat16)
            deg[band] += jnp.sum(weights.reshape(BAND // 8, 8, BAND), axis=0)
        copy_of(group).start()
        return carry

    lax.fori_loop(0, groups, body, 0)
    for back in range(STAGES, 0, -1):
        @pl.when(groups >= back)
        def _():
            copy_of(groups - back).wait()


def local_kernel(work, count, rows, sides, rvec, tiles, deg, cols, stage, sems):
    deg[...] = jnp.zeros(deg.shape, deg.dtype)

    def fill(band, carry):
        cols[band] = spread_column(sides[band])
        return carry

    lax.fori_loop(0, rows.shape[0], fill, 0, unroll=4)
    tile_groups(work, count, rows, lambda entry: rows[entry], cols, rvec, tiles, deg, stage, sems)


def pack_rows(send_index, scaled, send):
    def one(at, carry):
        send[at] = scaled[send_index[at]]
        return carry

    lax.fori_loop(0, send.shape[0], one, 0, unroll=8)


def remote_kernel(work, count, send_index, rows, got, rvec, deg_in, start,
                  tiles, root, scaled, send, deg, cols, stage, sems):
    deg[...] = deg_in[...]
    tail = MOST * BAND

    def fill(owner, carry):
        for h in range(MOST):
            side = got[owner, tail : tail + EXTRA, h * BAND : (h + 1) * BAND]
            cols[owner * MOST + h] = spread_column(side)
        return carry

    lax.fori_loop(0, got.shape[0], fill, 0, unroll=4)

    def coords_of(entry):
        at = pl.multiple_of(lax.rem(entry, MOST) * BAND, BAND)
        return got[entry // MOST, pl.ds(at, BAND), :]

    tile_groups(work, count, rows, coords_of, cols, rvec, tiles, deg, stage, sems)
    for band in range(deg.shape[0]):
        total = jnp.sum(deg[band], axis=0, keepdims=True)
        inverse = 1.0 / jnp.sqrt(total)
        root[band : band + 1, :] = inverse
        block = start[:, band * BAND : (band + 1) * BAND]
        scaled[band] = (block * inverse).astype(jnp.bfloat16)
    pack_rows(send_index, scaled, send)


def gather_product(work, count, table, tiles, total, held, sems):
    groups = (count[0] + GROUP - 1) // GROUP

    def copy_of(group):
        part = pl.ds(group * GROUP, GROUP)
        return pltpu.make_async_copy(tiles.at[part], held.at[part], sems.at[group])

    def begin(group, carry):
        copy_of(group).start()
        return carry

    def body(group, carry):
        copy_of(group).wait()
        for u in range(GROUP):
            at = group * GROUP + u
            total[work[0, at]] += jnp.dot(
                table[work[1, at]], held[at], preferred_element_type=jnp.float32
            )
        return carry

    lax.fori_loop(0, groups, begin, 0)
    lax.fori_loop(0, groups, body, 0)


def own_kernel(work, count, scaled, tiles, total, held, sems):
    total[...] = jnp.zeros(total.shape, total.dtype)
    gather_product(work, count, scaled, tiles, total, held, sems)


def fold(square):
    return jnp.concatenate([square[8 * q : 8 * q + 8, :] for q in range(square.shape[0] // 8)], axis=1)


def unfold(packed, side):
    return jnp.concatenate([packed[:, side * q : side * (q + 1)] for q in range(side // 8)], axis=0)


def round_kernel(first, last, gains, work, count, send_index, got, total_in, root, cur, prev, tiles,
                 following, *rest):
    if last:
        gram, total, held, sems = rest
    else:
        scaled, send, total, held, sems = rest
    total[...] = total_in[...]
    gather_product(work, count, got, tiles, total, held, sems)
    own, mixed_gain, old = gains
    for band in range(total.shape[0]):
        inverse = root[band : band + 1, :]
        lanes = slice(band * BAND, (band + 1) * BAND)
        block = own * cur[:, lanes] + (mixed_gain * inverse) * total[band]
        if not first:
            block = block - old * prev[:, lanes]
        following[:, lanes] = block
        if not last:
            scaled[band] = (inverse * block).astype(jnp.bfloat16)
    if last:
        piece = following[...]
        square = lax.dot_general(
            piece, piece, (((1,), (1,)), ((), ())),
            precision=lax.Precision.HIGHEST, preferred_element_type=jnp.float32,
        )
        gram[...] = jnp.broadcast_to(fold(square)[None], gram.shape)
    else:
        pack_rows(send_index, scaled, send)


def finish_kernel(total_rows, parts, flat, basis, factor):
    vectors = flat.shape[0]
    gram = unfold(jnp.sum(parts[...], axis=0), vectors) / total_rows
    row_ids = lax.broadcasted_iota(jnp.int32, (vectors, vectors), 0)
    col_ids = lax.broadcasted_iota(jnp.int32, (vectors, vectors), 1)
    left = gram
    right = jnp.where(row_ids == col_ids, 1.0, 0.0).astype(jnp.float32)
    lower = jnp.zeros((vectors, vectors), jnp.float32)
    scale = jnp.zeros((vectors, 1), jnp.float32)
    rows = lax.broadcasted_iota(jnp.int32, (vectors, 1), 0)
    for j in range(vectors):
        pivot = left[j : j + 1, j : j + 1]
        inverse = 1.0 / pivot
        column = left[:, j : j + 1]
        ratio = jnp.where(rows > j, column * inverse, 0.0)
        spread = 1.0 / jnp.sqrt(pivot)
        scale = jnp.where(rows == j, spread, scale)
        lower = jnp.where((col_ids == j) & (row_ids >= j), column * spread, lower)
        left_row = left[j : j + 1, :]
        right_row = right[j : j + 1, :]
        left = left - ratio * left_row
        right = right - ratio * right_row
    factor[...] = lower
    basis[...] = jnp.dot(
        right * scale, flat[...], precision=lax.Precision.HIGHEST, preferred_element_type=jnp.float32
    )


def on_device(features, inv_width, start_block, neighbour_ids, slot_mask):
    bands, slots = neighbour_ids.shape
    dims = features.shape[1]
    vectors = start_block.shape[0]
    devices = lax.axis_size(AXES)
    device = lax.axis_index(AXES)
    entries = devices * MOST
    count_all = bands * slots

    ids = neighbour_ids.T
    mask = slot_mask.T
    need_mine = pl.pallas_call(
        need_kernel,
        out_shape=jax.ShapeDtypeStruct((devices, bands), jnp.int32),
        in_specs=[whole()] * 2,
        out_specs=whole(),
        name="need",
    )(ids, mask)
    wanted = exchange(need_mine)
    rank_send = jnp.cumsum(wanted, axis=1) - 1
    picks = (wanted[:, None, :] == 1) & (
        rank_send[:, None, :] == jnp.arange(MOST, dtype=jnp.int32)[None, :, None]
    )
    send_index = jnp.sum(
        picks.astype(jnp.int32) * jnp.arange(bands, dtype=jnp.int32)[None, None, :], axis=2
    ).reshape(-1)

    feature_bands = features.reshape(bands, BAND, dims)
    widths = inv_width.reshape(bands, BAND).astype(jnp.float32)
    squares = jnp.sum(jnp.square(feature_bands.astype(jnp.float32)), axis=2)
    product = 0.5 * squares * widths
    high = lax.reduce_precision(product, 8, 7)
    rest = product - high
    middle = lax.reduce_precision(rest, 8, 7)
    blank = jnp.zeros_like(widths)
    sides = jnp.stack(
        [widths, high, middle, rest - middle] + [blank] * (EXTRA - 4), axis=1
    ).astype(jnp.bfloat16)
    send_coords = pl.pallas_call(
        pack_kernel,
        out_shape=jax.ShapeDtypeStruct((devices, MOST * BAND + EXTRA, dims), jnp.bfloat16),
        in_specs=[whole(SMEM)] + [whole()] * 2,
        out_specs=whole(pl.ANY),
        scratch_shapes=[
            pltpu.VMEM((devices, EXTRA, dims), jnp.bfloat16),
            pltpu.SemaphoreType.DMA((MOST + 1, devices)),
        ],
        name="pack",
    )(send_index, feature_bands, sides)
    got_coords = exchange(send_coords)

    flat_ids = ids.reshape(-1)
    active = mask.reshape(-1) == 1
    owner_dev = flat_ids // bands
    within = flat_ids % bands
    far = active & (owner_dev != device)
    rank_mine = jnp.cumsum(need_mine, axis=1) - 1
    rank_lookup = jnp.take(rank_mine.reshape(-1), flat_ids, axis=0, mode="clip")
    entry_of = jnp.where(far, owner_dev * MOST + rank_lookup, within)
    order = jnp.arange(count_all, dtype=jnp.int32)

    def work_list(chosen):
        ones = chosen.astype(jnp.int32)
        place = jnp.cumsum(ones) - 1
        hit = ((place[None, :] == order[:, None]) & chosen[None, :]).astype(jnp.int32)
        tile_id = jnp.sum(hit * order[None, :], axis=1)
        entry = jnp.sum(hit * entry_of[None, :], axis=1)
        count = jnp.sum(ones)
        keep = (order < count).astype(jnp.int32)
        return jnp.stack([tile_id % bands, entry, keep]), count.reshape(1)

    near_work, near_count = work_list(active & ~far)
    far_work, far_count = work_list(far)

    rvec = jnp.stack([0.5 * squares, (2.0 * math.log2(math.e)) * widths], axis=1)

    tile_shape = jax.ShapeDtypeStruct((count_all, BAND, BAND), jnp.bfloat16)

    def building(columns):
        return [
            pltpu.VMEM((columns, BAND, 2 * BAND), jnp.float32),
            pltpu.VMEM((STAGES, GROUP, BAND, BAND), jnp.bfloat16),
            pltpu.SemaphoreType.DMA((STAGES,)),
        ]

    remote_bytes = entries * BAND * (8 * BAND + 3 * dims) + 10 * 1024 * 1024
    tile_area = count_all * BAND * BAND
    build_cost = pl.CostEstimate(
        flops=tile_area * dims, bytes_accessed=tile_area, transcendentals=tile_area // 2
    )
    near_tiles, deg = pl.pallas_call(
        local_kernel,
        out_shape=(tile_shape, jax.ShapeDtypeStruct((bands, 8, BAND), jnp.float32)),
        in_specs=[whole(SMEM)] * 2 + [whole()] * 3,
        out_specs=(whole(pl.ANY), whole()),
        scratch_shapes=building(bands),
        cost_estimate=build_cost,
        compiler_params=pltpu.CompilerParams(vmem_limit_bytes=LIMIT),
        name="local_tiles",
    )(near_work, near_count, feature_bands, sides, rvec)

    row_shape = jax.ShapeDtypeStruct((bands, vectors, BAND), jnp.bfloat16)
    send_shape = jax.ShapeDtypeStruct((entries, vectors, BAND), jnp.bfloat16)
    far_tiles, root, scaled, send = pl.pallas_call(
        remote_kernel,
        out_shape=(tile_shape, jax.ShapeDtypeStruct((bands, BAND), jnp.float32), row_shape, send_shape),
        in_specs=[whole(SMEM)] * 3 + [whole()] * 5,
        out_specs=(whole(pl.ANY), whole(), whole(), whole()),
        scratch_shapes=[pltpu.VMEM((bands, 8, BAND), jnp.float32)] + building(entries),
        cost_estimate=build_cost,
        compiler_params=pltpu.CompilerParams(vmem_limit_bytes=max(LIMIT, remote_bytes)),
        name="remote_tiles",
    )(far_work, far_count, send_index, feature_bands, got_coords, rvec, deg, start_block)

    centre, halfwidth, values = chebyshev_terms()
    flat_shape = jax.ShapeDtypeStruct((vectors, bands * BAND), jnp.float32)
    total_shape = jax.ShapeDtypeStruct((bands, vectors, BAND), jnp.float32)
    gram_shape = jax.ShapeDtypeStruct((devices, 8, vectors * vectors // 8), jnp.float32)
    fetching = [
        pltpu.VMEM((count_all, BAND, BAND), jnp.bfloat16),
        pltpu.SemaphoreType.DMA((count_all // GROUP,)),
    ]
    product_cost = pl.CostEstimate(
        flops=tile_area * vectors, bytes_accessed=tile_area, transcendentals=0
    )
    previous, current = start_block, start_block
    for power in range(DEGREE):
        first, last = power == 0, power == DEGREE - 1
        if first:
            lead, old = 1.0 / values[1], 0.0
        else:
            lead = 2.0 * values[power] / values[power + 1]
            old = values[power - 1] / values[power + 1]
        gains = (lead * (1.0 - centre) / halfwidth, -lead / halfwidth, old)
        got = exchange(send.reshape(devices, MOST, vectors, BAND)).reshape(entries, vectors, BAND)
        own_total = pl.pallas_call(
            own_kernel,
            out_shape=total_shape,
            in_specs=[whole(SMEM)] * 2 + [whole(), whole(pl.ANY)],
            out_specs=whole(),
            scratch_shapes=fetching,
            cost_estimate=product_cost,
            compiler_params=pltpu.CompilerParams(vmem_limit_bytes=LIMIT),
            name="own" + str(power),
        )(near_work, near_count, scaled, near_tiles)
        outs = (flat_shape, gram_shape) if last else (flat_shape, row_shape, send_shape)
        results = pl.pallas_call(
            functools.partial(round_kernel, first, last, gains),
            out_shape=outs,
            in_specs=[whole(SMEM)] * 3 + [whole()] * 5 + [whole(pl.ANY)],
            out_specs=tuple([whole()] * len(outs)),
            scratch_shapes=[pltpu.VMEM((bands, vectors, BAND), jnp.float32)] + fetching,
            cost_estimate=product_cost,
            compiler_params=pltpu.CompilerParams(vmem_limit_bytes=LIMIT),
            name="round" + str(power),
        )(far_work, far_count, send_index, got, own_total, root, current, previous, far_tiles)
        previous, current = current, results[0]
        if last:
            parts = exchange(results[1])
        else:
            scaled, send = results[1], results[2]

    basis, factor = pl.pallas_call(
        functools.partial(finish_kernel, devices * bands * BAND),
        out_shape=(flat_shape, jax.ShapeDtypeStruct((vectors, vectors), jnp.float32)),
        in_specs=[whole()] * 2,
        out_specs=(whole(), whole()),
        compiler_params=pltpu.CompilerParams(vmem_limit_bytes=LIMIT),
        name="finish",
    )(parts, current)
    return (basis, factor)


def solution(mesh):
    placed = (P(AXES, None), P(AXES), P(None, AXES), P(AXES, None), P(AXES, None))
    return jax.shard_map(
        on_device,
        mesh=mesh,
        in_specs=placed,
        out_specs=(P(None, AXES), P()),
        check_vma=False,
    )
```

```python
import functools
import math

import jax
import jax.numpy as jnp
from jax import lax
from jax.experimental import pallas as pl
from jax.experimental.pallas import tpu as pltpu
from jax.sharding import PartitionSpec as P

AXES = ("gx", "gy")
BAND = 128
MOST = 2
DEGREE = 4
GROUP = 16
STAGES = 4
EXTRA = 8
AHEAD = 8
LIMIT = 50 * 1024 * 1024

LOW_EDGE = 0.2
HIGH_EDGE = 2.0

VMEM = pltpu.VMEM
SMEM = pltpu.SMEM


def chebyshev_terms():
    centre = 0.5 * (LOW_EDGE + HIGH_EDGE)
    halfwidth = 0.5 * (HIGH_EDGE - LOW_EDGE)
    anchor = -centre / halfwidth
    values = [1.0, anchor]
    for repeat in range(DEGREE - 1):
        values.append(2.0 * anchor * values[-1] - values[-2])
    return (centre, halfwidth, values)


def exchange(blocks):
    return lax.all_to_all(blocks, AXES, split_axis=0, concat_axis=0, tiled=True)


def whole(space=VMEM):
    return pl.BlockSpec(memory_space=space)


def need_kernel(ids, mask, need):
    slots, bands = ids.shape
    devices = need.shape[0]
    device_ids = lax.broadcasted_iota(jnp.int32, (devices, bands), 0)
    band_ids = lax.broadcasted_iota(jnp.int32, (bands, bands), 0)
    owners, withins = [], []
    for j in range(slots):
        row = ids[j : j + 1, :]
        keep = mask[j : j + 1, :] == 1
        owners.append(jnp.where((row // bands == device_ids) & keep, 1.0, 0.0))
        withins.append(jnp.where(row % bands == band_ids, 1.0, 0.0))
    count = lax.dot_general(
        jnp.concatenate(owners, axis=1).astype(jnp.bfloat16),
        jnp.concatenate(withins, axis=1).astype(jnp.bfloat16),
        (((1,), (1,)), ((), ())),
        preferred_element_type=jnp.float32,
    )
    need[...] = jnp.where(count > 0.0, 1, 0).astype(jnp.int32)


def pack_kernel(send_index, features, sides, send, tails, sems):
    devices = send.shape[0]

    def bands_of(d):
        return [
            pltpu.make_async_copy(
                features.at[send_index[d, h]],
                send.at[d, pl.ds(h * BAND, BAND)],
                sems.at[h, d],
            )
            for h in range(MOST)
        ]

    def tail_of(d):
        return pltpu.make_async_copy(
            tails.at[d], send.at[d, pl.ds(MOST * BAND, EXTRA)], sems.at[MOST, d]
        )

    def first(d, carry):
        for copy in bands_of(d):
            copy.start()
        tails[d] = jnp.concatenate([sides[send_index[d, h]] for h in range(MOST)], axis=1)
        return carry

    def second(d, carry):
        tail_of(d).start()
        return carry

    def third(d, carry):
        for copy in bands_of(d):
            copy.wait()
        tail_of(d).wait()
        return carry

    lax.fori_loop(0, devices, first, 0)
    lax.fori_loop(0, devices, second, 0)
    lax.fori_loop(0, devices, third, 0)


def spread_column(side):
    row = lax.broadcasted_iota(jnp.int32, (EXTRA, 2 * BAND), 0)
    lane = lax.broadcasted_iota(jnp.int32, (EXTRA, 2 * BAND), 1)
    left = jnp.where((row == 0) & (lane < BAND), 1.0, 0.0)
    right = jnp.where((row > 0) & (row < 4) & (lane >= BAND), 1.0, 0.0)
    return lax.dot_general(
        side, (left + right).astype(jnp.bfloat16), (((0,), (0,)), ((), ())),
        preferred_element_type=jnp.float32,
    )


def tile_groups(work, rows, coords_of, cols, rvec, tiles, deg, stage, sems, between):
    groups = (work[3, 0] + GROUP - 1) // GROUP

    def copy_of(group):
        slot = lax.rem(group, STAGES)
        return pltpu.make_async_copy(
            stage.at[slot], tiles.at[pl.ds(group * GROUP, GROUP)], sems.at[slot]
        )

    def body(group, carry):
        slot = lax.rem(group, STAGES)

        @pl.when(group >= STAGES)
        def _():
            copy_of(group - STAGES).wait()

        for u in range(GROUP):
            at = group * GROUP + u
            band = work[0, at]
            entry = work[1, at]
            keep = work[2, at].astype(jnp.float32)
            inner = lax.dot_general(
                coords_of(entry), rows[band], (((1,), (1,)), ((), ())),
                preferred_element_type=jnp.float32,
            )
            half_sq = rvec[band, 0:1, :]
            row_width = rvec[band, 1:2, :]
            power = ((inner - half_sq) * cols[entry, :, 0:BAND] - cols[entry, :, BAND:]) * row_width
            weights = jnp.exp2(power) * keep
            stage[slot, u] = weights.astype(jnp.bfloat16)
            deg[band] += jnp.sum(weights.reshape(BAND // 8, 8, BAND), axis=0)
        copy_of(group).start()
        return carry

    lax.fori_loop(0, groups, body, 0)
    between()
    for back in range(STAGES, 0, -1):
        @pl.when(groups >= back)
        def _():
            copy_of(groups - back).wait()


def local_kernel(work, rows, sides, rvec, tiles, deg, cols, stage, sems):
    deg[...] = jnp.zeros(deg.shape, deg.dtype)

    def fill(band, carry):
        cols[band] = spread_column(sides[band])
        return carry

    lax.fori_loop(0, rows.shape[0], fill, 0, unroll=4)
    tile_groups(work, rows, lambda entry: rows[entry], cols, rvec, tiles, deg, stage, sems, lambda: None)


def pack_rows(work, scaled, send):
    def one(at, carry):
        send[at] = scaled[work[4, at]]
        return carry

    lax.fori_loop(0, send.shape[0], one, 0, unroll=8)


def remote_kernel(work_in, rows, got_in, rvec, deg_in, start,
                  tiles, root, scaled, send, work, got, deg, cols, stage, sems, work_sem, got_sems):
    work_copy = pltpu.make_async_copy(work_in, work, work_sem)
    work_copy.start()

    def copy_of(owner):
        return pltpu.make_async_copy(got_in.at[owner], got.at[owner], got_sems.at[owner])

    def begin(owner, carry):
        copy_of(owner).start()
        return carry

    lax.fori_loop(0, got.shape[0], begin, 0)
    deg[...] = deg_in[...]
    tail = MOST * BAND
    step = 4

    def fill(part, carry):
        for k in range(step):
            copy_of(part * step + k).wait()
        for k in range(step):
            owner = part * step + k
            for h in range(MOST):
                side = got[owner, tail : tail + EXTRA, h * BAND : (h + 1) * BAND]
                cols[owner * MOST + h] = spread_column(side)
        return carry

    lax.fori_loop(0, got.shape[0] // step, fill, 0)
    work_copy.wait()

    def coords_of(entry):
        at = pl.multiple_of(lax.rem(entry, MOST) * BAND, BAND)
        return got[entry // MOST, pl.ds(at, BAND), :]

    def between():
        for band in range(deg.shape[0]):
            total = jnp.sum(deg[band], axis=0, keepdims=True)
            inverse = 1.0 / jnp.sqrt(total)
            root[band : band + 1, :] = inverse
            block = start[:, band * BAND : (band + 1) * BAND]
            scaled[band] = (block * inverse).astype(jnp.bfloat16)
        pack_rows(work, scaled, send)

    tile_groups(work, rows, coords_of, cols, rvec, tiles, deg, stage, sems, between)


def gather_product(work_in, table, tiles, total, work, held, work_sem, sems):
    work_copy = pltpu.make_async_copy(work_in, work, work_sem)

    def copy_of(group):
        part = pl.ds(group * GROUP, GROUP)
        return pltpu.make_async_copy(tiles.at[part], held.at[part], sems.at[group])

    def begin(group, carry):
        copy_of(group).start()
        return carry

    def body(group, carry):
        copy_of(group).wait()
        for u in range(GROUP):
            at = group * GROUP + u
            total[work[0, at]] += jnp.dot(
                table[work[1, at]], held[at], preferred_element_type=jnp.float32
            )
        return carry

    def spare(group, carry):
        copy_of(group).wait()
        return carry

    ahead = min(AHEAD, sems.shape[0])
    work_copy.start()
    for group in range(ahead):
        copy_of(group).start()
    work_copy.wait()
    groups = (work[3, 0] + GROUP - 1) // GROUP
    lax.fori_loop(ahead, groups, begin, 0)
    lax.fori_loop(0, groups, body, 0)
    lax.fori_loop(groups, ahead, spare, 0)


def own_kernel(work_in, scaled, tiles, total, work, held, work_sem, sems):
    total[...] = jnp.zeros(total.shape, total.dtype)
    gather_product(work_in, scaled, tiles, total, work, held, work_sem, sems)


def fold(square):
    return jnp.concatenate([square[8 * q : 8 * q + 8, :] for q in range(square.shape[0] // 8)], axis=1)


def unfold(packed, side):
    return jnp.concatenate([packed[:, side * q : side * (q + 1)] for q in range(side // 8)], axis=0)


def round_kernel(first, last, gains, work_in, got, total_in, root, cur, prev, tiles, following, *rest):
    if last:
        gram, total, work, held, work_sem, sems = rest
    else:
        scaled, send, total, work, held, work_sem, sems = rest
    total[...] = total_in[...]
    gather_product(work_in, got, tiles, total, work, held, work_sem, sems)
    own, mixed_gain, old = gains
    for band in range(total.shape[0]):
        inverse = root[band : band + 1, :]
        lanes = slice(band * BAND, (band + 1) * BAND)
        block = own * cur[:, lanes] + (mixed_gain * inverse) * total[band]
        if not first:
            block = block - old * prev[:, lanes]
        following[:, lanes] = block
        if not last:
            scaled[band] = (inverse * block).astype(jnp.bfloat16)
    if last:
        piece = following[...]
        square = lax.dot_general(
            piece, piece, (((1,), (1,)), ((), ())),
            precision=lax.Precision.HIGHEST, preferred_element_type=jnp.float32,
        )
        gram[...] = jnp.broadcast_to(fold(square)[None], gram.shape)
    else:
        pack_rows(work, scaled, send)


def finish_kernel(total_rows, parts, flat, basis, factor):
    vectors = flat.shape[0]
    gram = unfold(jnp.sum(parts[...], axis=0), vectors) / total_rows
    row_ids = lax.broadcasted_iota(jnp.int32, (vectors, vectors), 0)
    col_ids = lax.broadcasted_iota(jnp.int32, (vectors, vectors), 1)
    left = gram
    right = jnp.where(row_ids == col_ids, 1.0, 0.0).astype(jnp.float32)
    lower = jnp.zeros((vectors, vectors), jnp.float32)
    scale = jnp.zeros((vectors, 1), jnp.float32)
    rows = lax.broadcasted_iota(jnp.int32, (vectors, 1), 0)
    for j in range(vectors):
        pivot = left[j : j + 1, j : j + 1]
        inverse = 1.0 / pivot
        column = left[:, j : j + 1]
        ratio = jnp.where(rows > j, column * inverse, 0.0)
        spread = 1.0 / jnp.sqrt(pivot)
        scale = jnp.where(rows == j, spread, scale)
        lower = jnp.where((col_ids == j) & (row_ids >= j), column * spread, lower)
        left_row = left[j : j + 1, :]
        right_row = right[j : j + 1, :]
        left = left - ratio * left_row
        right = right - ratio * right_row
    factor[...] = lower
    basis[...] = jnp.dot(
        right * scale, flat[...], precision=lax.Precision.HIGHEST, preferred_element_type=jnp.float32
    )


def on_device(features, inv_width, start_block, neighbour_ids, slot_mask):
    bands, slots = neighbour_ids.shape
    dims = features.shape[1]
    vectors = start_block.shape[0]
    devices = lax.axis_size(AXES)
    device = lax.axis_index(AXES)
    entries = devices * MOST
    count_all = bands * slots

    ids = neighbour_ids.T
    mask = slot_mask.T
    need_mine = pl.pallas_call(
        need_kernel,
        out_shape=jax.ShapeDtypeStruct((devices, bands), jnp.int32),
        in_specs=[whole()] * 2,
        out_specs=whole(),
        name="need",
    )(ids, mask)
    wanted = exchange(need_mine)
    rank_send = jnp.cumsum(wanted, axis=1) - 1
    picks = (wanted[:, None, :] == 1) & (
        rank_send[:, None, :] == jnp.arange(MOST, dtype=jnp.int32)[None, :, None]
    )
    send_index = jnp.sum(
        picks.astype(jnp.int32) * jnp.arange(bands, dtype=jnp.int32)[None, None, :], axis=2
    )

    feature_bands = features.reshape(bands, BAND, dims)
    widths = inv_width.reshape(bands, BAND).astype(jnp.float32)
    squares = jnp.sum(jnp.square(feature_bands.astype(jnp.float32)), axis=2)
    product = 0.5 * squares * widths
    high = lax.reduce_precision(product, 8, 7)
    rest = product - high
    middle = lax.reduce_precision(rest, 8, 7)
    blank = jnp.zeros_like(widths)
    sides = jnp.stack(
        [widths, high, middle, rest - middle] + [blank] * (EXTRA - 4), axis=1
    ).astype(jnp.bfloat16)
    send_coords = pl.pallas_call(
        pack_kernel,
        out_shape=jax.ShapeDtypeStruct((devices, MOST * BAND + EXTRA, dims), jnp.bfloat16),
        in_specs=[whole(SMEM)] + [whole()] * 2,
        out_specs=whole(pl.ANY),
        scratch_shapes=[
            pltpu.VMEM((devices, EXTRA, dims), jnp.bfloat16),
            pltpu.SemaphoreType.DMA((MOST + 1, devices)),
        ],
        compiler_params=pltpu.CompilerParams(vmem_limit_bytes=LIMIT),
        name="pack",
    )(send_index, feature_bands, sides)
    got_coords = exchange(send_coords)

    flat_ids = ids.reshape(-1)
    active = mask.reshape(-1) == 1
    owner_dev = flat_ids // bands
    within = flat_ids % bands
    far = active & (owner_dev != device)
    rank_mine = jnp.cumsum(need_mine, axis=1) - 1
    rank_lookup = jnp.take(rank_mine.reshape(-1), flat_ids, axis=0, mode="clip")
    entry_of = jnp.where(far, owner_dev * MOST + rank_lookup, within)
    order = jnp.arange(count_all, dtype=jnp.int32)

    def work_list(chosen):
        ones = chosen.astype(jnp.int32)
        place = jnp.cumsum(ones) - 1
        hit = ((place[None, :] == order[:, None]) & chosen[None, :]).astype(jnp.int32)
        tile_id = jnp.sum(hit * order[None, :], axis=1)
        entry = jnp.sum(hit * entry_of[None, :], axis=1)
        count = jnp.sum(ones)
        keep = (order < count).astype(jnp.int32)
        rows = jnp.stack([tile_id % bands, entry, keep, jnp.broadcast_to(count, order.shape)])
        rows = jnp.pad(rows, ((0, 0), (0, width - count_all)))
        return jnp.concatenate([rows, send_row], axis=0)

    width = -(-max(count_all, entries) // BAND) * BAND
    send_row = jnp.pad(send_index.reshape(1, entries), ((0, 0), (0, width - entries)))
    near_work = work_list(active & ~far)
    far_work = work_list(far)

    rvec = jnp.stack([0.5 * squares, (2.0 * math.log2(math.e)) * widths], axis=1)

    work_space = pltpu.SMEM(far_work.shape, jnp.int32)
    tile_shape = jax.ShapeDtypeStruct((count_all, BAND, BAND), jnp.bfloat16)

    def building(columns):
        return [
            pltpu.VMEM((columns, BAND, 2 * BAND), jnp.float32),
            pltpu.VMEM((STAGES, GROUP, BAND, BAND), jnp.bfloat16),
            pltpu.SemaphoreType.DMA((STAGES,)),
        ]

    remote_bytes = entries * BAND * (8 * BAND + 3 * dims) + 10 * 1024 * 1024
    tile_area = count_all * BAND * BAND
    build_cost = pl.CostEstimate(
        flops=tile_area * dims, bytes_accessed=tile_area, transcendentals=tile_area // 2
    )
    near_tiles, deg = pl.pallas_call(
        local_kernel,
        out_shape=(tile_shape, jax.ShapeDtypeStruct((bands, 8, BAND), jnp.float32)),
        in_specs=[whole(SMEM)] + [whole()] * 3,
        out_specs=(whole(pl.ANY), whole()),
        scratch_shapes=building(bands),
        cost_estimate=build_cost,
        compiler_params=pltpu.CompilerParams(vmem_limit_bytes=LIMIT),
        name="local_tiles",
    )(near_work, feature_bands, sides, rvec)

    row_shape = jax.ShapeDtypeStruct((bands, vectors, BAND), jnp.bfloat16)
    send_shape = jax.ShapeDtypeStruct((entries, vectors, BAND), jnp.bfloat16)
    far_tiles, root, scaled, send = pl.pallas_call(
        remote_kernel,
        out_shape=(tile_shape, jax.ShapeDtypeStruct((bands, BAND), jnp.float32), row_shape, send_shape),
        in_specs=[whole(pltpu.HBM), whole(), whole(pltpu.HBM)] + [whole()] * 3,
        out_specs=(whole(pl.ANY), whole(), whole(), whole()),
        scratch_shapes=[
            work_space,
            pltpu.VMEM(send_coords.shape, jnp.bfloat16),
            pltpu.VMEM((bands, 8, BAND), jnp.float32),
        ] + building(entries) + [pltpu.SemaphoreType.DMA, pltpu.SemaphoreType.DMA((devices,))],
        cost_estimate=build_cost,
        compiler_params=pltpu.CompilerParams(vmem_limit_bytes=max(LIMIT, remote_bytes)),
        name="remote_tiles",
    )(far_work, feature_bands, got_coords, rvec, deg, start_block)

    centre, halfwidth, values = chebyshev_terms()
    flat_shape = jax.ShapeDtypeStruct((vectors, bands * BAND), jnp.float32)
    total_shape = jax.ShapeDtypeStruct((bands, vectors, BAND), jnp.float32)
    gram_shape = jax.ShapeDtypeStruct((devices, 8, vectors * vectors // 8), jnp.float32)
    fetching = [
        work_space,
        pltpu.VMEM((count_all, BAND, BAND), jnp.bfloat16),
        pltpu.SemaphoreType.DMA,
        pltpu.SemaphoreType.DMA((count_all // GROUP,)),
    ]
    product_cost = pl.CostEstimate(
        flops=tile_area * vectors, bytes_accessed=tile_area, transcendentals=0
    )
    previous, current = start_block, start_block
    for power in range(DEGREE):
        first, last = power == 0, power == DEGREE - 1
        if first:
            lead, old = 1.0 / values[1], 0.0
        else:
            lead = 2.0 * values[power] / values[power + 1]
            old = values[power - 1] / values[power + 1]
        gains = (lead * (1.0 - centre) / halfwidth, -lead / halfwidth, old)
        got = exchange(send.reshape(devices, MOST, vectors, BAND)).reshape(entries, vectors, BAND)
        own_total = pl.pallas_call(
            own_kernel,
            out_shape=total_shape,
            in_specs=[whole(pltpu.HBM), whole(), whole(pltpu.HBM)],
            out_specs=whole(),
            scratch_shapes=fetching,
            cost_estimate=product_cost,
            compiler_params=pltpu.CompilerParams(vmem_limit_bytes=LIMIT),
            name="own" + str(power),
        )(near_work, scaled, near_tiles)
        outs = (flat_shape, gram_shape) if last else (flat_shape, row_shape, send_shape)
        results = pl.pallas_call(
            functools.partial(round_kernel, first, last, gains),
            out_shape=outs,
            in_specs=[whole(pltpu.HBM)] + [whole()] * 5 + [whole(pltpu.HBM)],
            out_specs=tuple([whole()] * len(outs)),
            scratch_shapes=[pltpu.VMEM((bands, vectors, BAND), jnp.float32)] + fetching,
            cost_estimate=product_cost,
            compiler_params=pltpu.CompilerParams(vmem_limit_bytes=LIMIT),
            name="round" + str(power),
        )(far_work, got, own_total, root, current, previous, far_tiles)
        previous, current = current, results[0]
        if last:
            parts = exchange(results[1])
        else:
            scaled, send = results[1], results[2]

    basis, factor = pl.pallas_call(
        functools.partial(finish_kernel, devices * bands * BAND),
        out_shape=(flat_shape, jax.ShapeDtypeStruct((vectors, vectors), jnp.float32)),
        in_specs=[whole()] * 2,
        out_specs=(whole(), whole()),
        compiler_params=pltpu.CompilerParams(vmem_limit_bytes=LIMIT),
        name="finish",
    )(parts, current)
    return (basis, factor)


def solution(mesh):
    placed = (P(AXES, None), P(AXES), P(None, AXES), P(AXES, None), P(AXES, None))
    return jax.shard_map(
        on_device,
        mesh=mesh,
        in_specs=placed,
        out_specs=(P(None, AXES), P()),
        check_vma=False,
    )
```

```python
import functools
import math

import jax
import jax.numpy as jnp
from jax import lax
from jax.experimental import pallas as pl
from jax.experimental.pallas import tpu as pltpu
from jax.sharding import PartitionSpec as P

AXES = ("gx", "gy")
BAND = 128
MOST = 2
DEGREE = 4
GROUP = 32
STAGES = 3
EXTRA = 8
AHEAD = 4
LIMIT = 50 * 1024 * 1024

LOW_EDGE = 0.2
HIGH_EDGE = 2.0

VMEM = pltpu.VMEM
SMEM = pltpu.SMEM


def chebyshev_terms():
    centre = 0.5 * (LOW_EDGE + HIGH_EDGE)
    halfwidth = 0.5 * (HIGH_EDGE - LOW_EDGE)
    anchor = -centre / halfwidth
    values = [1.0, anchor]
    for repeat in range(DEGREE - 1):
        values.append(2.0 * anchor * values[-1] - values[-2])
    return (centre, halfwidth, values)


def exchange(blocks):
    return lax.all_to_all(blocks, AXES, split_axis=0, concat_axis=0, tiled=True)


def whole(space=VMEM):
    return pl.BlockSpec(memory_space=space)


def need_kernel(ids, mask, need):
    slots, bands = ids.shape
    devices = need.shape[0]
    device_ids = lax.broadcasted_iota(jnp.int32, (devices, bands), 0)
    band_ids = lax.broadcasted_iota(jnp.int32, (bands, bands), 0)
    owners, withins = [], []
    for j in range(slots):
        row = ids[j : j + 1, :]
        keep = mask[j : j + 1, :] == 1
        owners.append(jnp.where((row // bands == device_ids) & keep, 1.0, 0.0))
        withins.append(jnp.where(row % bands == band_ids, 1.0, 0.0))
    count = lax.dot_general(
        jnp.concatenate(owners, axis=1).astype(jnp.bfloat16),
        jnp.concatenate(withins, axis=1).astype(jnp.bfloat16),
        (((1,), (1,)), ((), ())),
        preferred_element_type=jnp.float32,
    )
    need[...] = jnp.where(count > 0.0, 1, 0).astype(jnp.int32)


def sides_kernel(features, widths, copied, sides, rvec):
    dims = features.shape[2]
    ones = jnp.ones((EXTRA, dims), jnp.bfloat16)
    row = lax.broadcasted_iota(jnp.int32, (EXTRA, BAND), 0)

    def row_sums(part):
        return lax.dot_general(
            ones, part, (((1,), (1,)), ((), ())), preferred_element_type=jnp.float32
        )

    for band in range(features.shape[0]):
        block = features[band]
        copied[band] = block
        wide = block.astype(jnp.float32)
        exact = wide * wide
        high = exact.astype(jnp.bfloat16)
        low = (exact - high.astype(jnp.float32)).astype(jnp.bfloat16)
        half = 0.5 * (row_sums(high) + row_sums(low))
        width = jnp.broadcast_to(widths[band : band + 1, :], (EXTRA, BAND))
        product = half * width
        first = product.astype(jnp.bfloat16).astype(jnp.float32)
        left = product - first
        second = left.astype(jnp.bfloat16).astype(jnp.float32)
        third = left - second
        side = jnp.where(row == 0, width, jnp.where(row == 1, first, 0.0))
        side = jnp.where(row == 2, second, jnp.where(row == 3, third, side))
        sides[band] = side.astype(jnp.bfloat16)
        rvec[band] = jnp.where(row == 0, half, (2.0 * math.log2(math.e)) * width)


def pack_kernel(send_index, features, sides, send, tails, sems):
    devices = send.shape[0]

    def bands_of(d):
        return [
            pltpu.make_async_copy(
                features.at[send_index[d, h]],
                send.at[d, pl.ds(h * BAND, BAND)],
                sems.at[h, d],
            )
            for h in range(MOST)
        ]

    def tail_of(d):
        return pltpu.make_async_copy(
            tails.at[d], send.at[d, pl.ds(MOST * BAND, EXTRA)], sems.at[MOST, d]
        )

    def first(d, carry):
        for copy in bands_of(d):
            copy.start()
        tails[d] = jnp.concatenate([sides[send_index[d, h]] for h in range(MOST)], axis=1)
        return carry

    def second(d, carry):
        tail_of(d).start()
        return carry

    def third(d, carry):
        for copy in bands_of(d):
            copy.wait()
        tail_of(d).wait()
        return carry

    lax.fori_loop(0, devices, first, 0)
    lax.fori_loop(0, devices, second, 0)
    lax.fori_loop(0, devices, third, 0)


def spread_column(side):
    row = lax.broadcasted_iota(jnp.int32, (EXTRA, 2 * BAND), 0)
    lane = lax.broadcasted_iota(jnp.int32, (EXTRA, 2 * BAND), 1)
    left = jnp.where((row == 0) & (lane < BAND), 1.0, 0.0)
    right = jnp.where((row > 0) & (row < 4) & (lane >= BAND), 1.0, 0.0)
    return lax.dot_general(
        side, (left + right).astype(jnp.bfloat16), (((0,), (0,)), ((), ())),
        preferred_element_type=jnp.float32,
    )


def tile_groups(work, rows, coords_of, cols, rvec, tiles, deg, stage, sems, between):
    groups = (work[3, 0] + GROUP - 1) // GROUP

    def copy_of(group):
        slot = lax.rem(group, STAGES)
        return pltpu.make_async_copy(
            stage.at[slot], tiles.at[pl.ds(group * GROUP, GROUP)], sems.at[slot]
        )

    def body(group, carry):
        slot = lax.rem(group, STAGES)

        @pl.when(group >= STAGES)
        def _():
            copy_of(group - STAGES).wait()

        for u in range(GROUP):
            at = group * GROUP + u
            band = work[0, at]
            entry = work[1, at]
            keep = work[2, at].astype(jnp.float32)
            inner = lax.dot_general(
                coords_of(entry), rows[band], (((1,), (1,)), ((), ())),
                preferred_element_type=jnp.float32,
            )
            half_sq = rvec[band, 0:1, :]
            row_width = rvec[band, 1:2, :]
            power = ((inner - half_sq) * cols[entry, :, 0:BAND] - cols[entry, :, BAND:]) * row_width
            weights = jnp.exp2(power) * keep
            stage[slot, u] = weights.astype(jnp.bfloat16)
            deg[band] += jnp.sum(weights.reshape(BAND // 8, 8, BAND), axis=0)
        copy_of(group).start()
        return carry

    lax.fori_loop(0, groups, body, 0)
    between()
    for back in range(STAGES, 0, -1):
        @pl.when(groups >= back)
        def _():
            copy_of(groups - back).wait()


def local_kernel(work, rows, sides, rvec, tiles, deg, cols, stage, sems):
    deg[...] = jnp.zeros(deg.shape, deg.dtype)

    def fill(band, carry):
        cols[band] = spread_column(sides[band])
        return carry

    lax.fori_loop(0, rows.shape[0], fill, 0, unroll=4)
    tile_groups(work, rows, lambda entry: rows[entry], cols, rvec, tiles, deg, stage, sems, lambda: None)


def pack_rows(work, scaled, send):
    def one(at, carry):
        send[at] = scaled[work[4, at]]
        return carry

    lax.fori_loop(0, send.shape[0], one, 0, unroll=8)


def remote_kernel(work_in, rows, got_in, rvec, deg_in, start,
                  tiles, root, scaled, send, work, got, deg, cols, stage, sems, work_sem, got_sems):
    work_copy = pltpu.make_async_copy(work_in, work, work_sem)
    work_copy.start()

    def copy_of(owner):
        return pltpu.make_async_copy(got_in.at[owner], got.at[owner], got_sems.at[owner])

    def begin(owner, carry):
        copy_of(owner).start()
        return carry

    lax.fori_loop(0, got.shape[0], begin, 0)
    deg[...] = deg_in[...]
    tail = MOST * BAND
    step = 4

    def fill(part, carry):
        for k in range(step):
            copy_of(part * step + k).wait()
        for k in range(step):
            owner = part * step + k
            for h in range(MOST):
                side = got[owner, tail : tail + EXTRA, h * BAND : (h + 1) * BAND]
                cols[owner * MOST + h] = spread_column(side)
        return carry

    lax.fori_loop(0, got.shape[0] // step, fill, 0)
    work_copy.wait()

    def coords_of(entry):
        at = pl.multiple_of(lax.rem(entry, MOST) * BAND, BAND)
        return got[entry // MOST, pl.ds(at, BAND), :]

    def between():
        for band in range(deg.shape[0]):
            total = jnp.sum(deg[band], axis=0, keepdims=True)
            inverse = 1.0 / jnp.sqrt(total)
            root[band : band + 1, :] = inverse
            block = start[:, band * BAND : (band + 1) * BAND]
            scaled[band] = (block * inverse).astype(jnp.bfloat16)
        pack_rows(work, scaled, send)

    tile_groups(work, rows, coords_of, cols, rvec, tiles, deg, stage, sems, between)


def gather_product(work_in, table, tiles, total, work, held, work_sem, sems):
    work_copy = pltpu.make_async_copy(work_in, work, work_sem)

    def copy_of(group):
        part = pl.ds(group * GROUP, GROUP)
        return pltpu.make_async_copy(tiles.at[part], held.at[part], sems.at[group])

    def begin(group, carry):
        copy_of(group).start()
        return carry

    def body(group, carry):
        copy_of(group).wait()
        for u in range(GROUP):
            at = group * GROUP + u
            total[work[0, at]] += jnp.dot(
                table[work[1, at]], held[at], preferred_element_type=jnp.float32
            )
        return carry

    def spare(group, carry):
        copy_of(group).wait()
        return carry

    ahead = min(AHEAD, sems.shape[0])
    work_copy.start()
    for group in range(ahead):
        copy_of(group).start()
    work_copy.wait()
    groups = (work[3, 0] + GROUP - 1) // GROUP
    lax.fori_loop(ahead, groups, begin, 0)
    lax.fori_loop(0, groups, body, 0)
    lax.fori_loop(groups, ahead, spare, 0)


def own_kernel(work_in, scaled, tiles, total, work, held, work_sem, sems):
    total[...] = jnp.zeros(total.shape, total.dtype)
    gather_product(work_in, scaled, tiles, total, work, held, work_sem, sems)


def fold(square):
    return jnp.concatenate([square[8 * q : 8 * q + 8, :] for q in range(square.shape[0] // 8)], axis=1)


def unfold(packed, side):
    return jnp.concatenate([packed[:, side * q : side * (q + 1)] for q in range(side // 8)], axis=0)


def round_kernel(first, last, gains, work_in, got, total_in, root, cur, prev, tiles, following, *rest):
    if last:
        gram, total, work, held, work_sem, sems = rest
    else:
        scaled, send, total, work, held, work_sem, sems = rest
    total[...] = total_in[...]
    gather_product(work_in, got, tiles, total, work, held, work_sem, sems)
    own, mixed_gain, old = gains
    for band in range(total.shape[0]):
        inverse = root[band : band + 1, :]
        lanes = slice(band * BAND, (band + 1) * BAND)
        block = own * cur[:, lanes] + (mixed_gain * inverse) * total[band]
        if not first:
            block = block - old * prev[:, lanes]
        following[:, lanes] = block
        if not last:
            scaled[band] = (inverse * block).astype(jnp.bfloat16)
    if last:
        piece = following[...]
        square = lax.dot_general(
            piece, piece, (((1,), (1,)), ((), ())),
            precision=lax.Precision.HIGHEST, preferred_element_type=jnp.float32,
        )
        gram[...] = jnp.broadcast_to(fold(square)[None], gram.shape)
    else:
        pack_rows(work, scaled, send)


def finish_kernel(total_rows, parts, flat, basis, factor):
    vectors = flat.shape[0]
    gram = unfold(jnp.sum(parts[...], axis=0), vectors) / total_rows
    row_ids = lax.broadcasted_iota(jnp.int32, (vectors, vectors), 0)
    col_ids = lax.broadcasted_iota(jnp.int32, (vectors, vectors), 1)
    left = gram
    right = jnp.where(row_ids == col_ids, 1.0, 0.0).astype(jnp.float32)
    lower = jnp.zeros((vectors, vectors), jnp.float32)
    scale = jnp.zeros((vectors, 1), jnp.float32)
    rows = lax.broadcasted_iota(jnp.int32, (vectors, 1), 0)
    for j in range(vectors):
        pivot = left[j : j + 1, j : j + 1]
        inverse = 1.0 / pivot
        column = left[:, j : j + 1]
        ratio = jnp.where(rows > j, column * inverse, 0.0)
        spread = 1.0 / jnp.sqrt(pivot)
        scale = jnp.where(rows == j, spread, scale)
        lower = jnp.where((col_ids == j) & (row_ids >= j), column * spread, lower)
        left_row = left[j : j + 1, :]
        right_row = right[j : j + 1, :]
        left = left - ratio * left_row
        right = right - ratio * right_row
    factor[...] = lower
    basis[...] = jnp.dot(
        right * scale, flat[...], precision=lax.Precision.HIGHEST, preferred_element_type=jnp.float32
    )


def on_device(features, inv_width, start_block, neighbour_ids, slot_mask):
    bands, slots = neighbour_ids.shape
    dims = features.shape[1]
    vectors = start_block.shape[0]
    devices = lax.axis_size(AXES)
    device = lax.axis_index(AXES)
    entries = devices * MOST
    count_all = bands * slots

    ids = neighbour_ids.T
    mask = slot_mask.T
    need_mine = pl.pallas_call(
        need_kernel,
        out_shape=jax.ShapeDtypeStruct((devices, bands), jnp.int32),
        in_specs=[whole()] * 2,
        out_specs=whole(),
        name="need",
    )(ids, mask)
    wanted = exchange(need_mine)
    rank_send = jnp.cumsum(wanted, axis=1) - 1
    picks = (wanted[:, None, :] == 1) & (
        rank_send[:, None, :] == jnp.arange(MOST, dtype=jnp.int32)[None, :, None]
    )
    send_index = jnp.sum(
        picks.astype(jnp.int32) * jnp.arange(bands, dtype=jnp.int32)[None, None, :], axis=2
    )

    feature_bands = features.reshape(bands, BAND, dims)
    widths = inv_width.reshape(bands, BAND).astype(jnp.float32)
    copied, sides, rvec = pl.pallas_call(
        sides_kernel,
        out_shape=(
            jax.ShapeDtypeStruct(feature_bands.shape, jnp.bfloat16),
            jax.ShapeDtypeStruct((bands, EXTRA, BAND), jnp.bfloat16),
            jax.ShapeDtypeStruct((bands, EXTRA, BAND), jnp.float32),
        ),
        in_specs=[whole()] * 2,
        out_specs=(whole(), whole(), whole()),
        compiler_params=pltpu.CompilerParams(vmem_limit_bytes=LIMIT),
        cost_estimate=pl.CostEstimate(
            flops=4 * bands * BAND * BAND * dims, bytes_accessed=4 * features.size, transcendentals=0
        ),
        name="sides",
    )(feature_bands, widths)
    send_coords = pl.pallas_call(
        pack_kernel,
        out_shape=jax.ShapeDtypeStruct((devices, MOST * BAND + EXTRA, dims), jnp.bfloat16),
        in_specs=[whole(SMEM)] + [whole()] * 2,
        out_specs=whole(pl.ANY),
        scratch_shapes=[
            pltpu.VMEM((devices, EXTRA, dims), jnp.bfloat16),
            pltpu.SemaphoreType.DMA((MOST + 1, devices)),
        ],
        compiler_params=pltpu.CompilerParams(vmem_limit_bytes=LIMIT),
        name="pack",
    )(send_index, copied, sides)
    got_coords = exchange(send_coords)

    flat_ids = ids.reshape(-1)
    active = mask.reshape(-1) == 1
    owner_dev = flat_ids // bands
    within = flat_ids % bands
    far = active & (owner_dev != device)
    rank_mine = jnp.cumsum(need_mine, axis=1) - 1
    rank_lookup = jnp.take(rank_mine.reshape(-1), flat_ids, axis=0, mode="clip")
    entry_of = jnp.where(far, owner_dev * MOST + rank_lookup, within)
    order = jnp.arange(count_all, dtype=jnp.int32)

    def work_list(chosen):
        ones = chosen.astype(jnp.int32)
        place = jnp.cumsum(ones) - 1
        hit = ((place[None, :] == order[:, None]) & chosen[None, :]).astype(jnp.int32)
        tile_id = jnp.sum(hit * order[None, :], axis=1)
        entry = jnp.sum(hit * entry_of[None, :], axis=1)
        count = jnp.sum(ones)
        keep = (order < count).astype(jnp.int32)
        rows = jnp.stack([tile_id % bands, entry, keep, jnp.broadcast_to(count, order.shape)])
        rows = jnp.pad(rows, ((0, 0), (0, width - count_all)))
        return jnp.concatenate([rows, send_row], axis=0)

    width = -(-max(count_all, entries) // BAND) * BAND
    send_row = jnp.pad(send_index.reshape(1, entries), ((0, 0), (0, width - entries)))
    near_work = work_list(active & ~far)
    far_work = work_list(far)

    work_space = pltpu.SMEM(far_work.shape, jnp.int32)
    tile_shape = jax.ShapeDtypeStruct((count_all, BAND, BAND), jnp.bfloat16)

    def building(columns):
        return [
            pltpu.VMEM((columns, BAND, 2 * BAND), jnp.float32),
            pltpu.VMEM((STAGES, GROUP, BAND, BAND), jnp.bfloat16),
            pltpu.SemaphoreType.DMA((STAGES,)),
        ]

    remote_bytes = entries * BAND * (8 * BAND + 3 * dims) + 10 * 1024 * 1024
    tile_area = count_all * BAND * BAND
    build_cost = pl.CostEstimate(
        flops=tile_area * dims, bytes_accessed=tile_area, transcendentals=tile_area // 2
    )
    near_tiles, deg = pl.pallas_call(
        local_kernel,
        out_shape=(tile_shape, jax.ShapeDtypeStruct((bands, 8, BAND), jnp.float32)),
        in_specs=[whole(SMEM)] + [whole()] * 3,
        out_specs=(whole(pl.ANY), whole()),
        scratch_shapes=building(bands),
        cost_estimate=build_cost,
        compiler_params=pltpu.CompilerParams(vmem_limit_bytes=LIMIT),
        name="local_tiles",
    )(near_work, feature_bands, sides, rvec)

    row_shape = jax.ShapeDtypeStruct((bands, vectors, BAND), jnp.bfloat16)
    send_shape = jax.ShapeDtypeStruct((entries, vectors, BAND), jnp.bfloat16)
    far_tiles, root, scaled, send = pl.pallas_call(
        remote_kernel,
        out_shape=(tile_shape, jax.ShapeDtypeStruct((bands, BAND), jnp.float32), row_shape, send_shape),
        in_specs=[whole(pltpu.HBM), whole(), whole(pltpu.HBM)] + [whole()] * 3,
        out_specs=(whole(pl.ANY), whole(), whole(), whole()),
        scratch_shapes=[
            work_space,
            pltpu.VMEM(send_coords.shape, jnp.bfloat16),
            pltpu.VMEM((bands, 8, BAND), jnp.float32),
        ] + building(entries) + [pltpu.SemaphoreType.DMA, pltpu.SemaphoreType.DMA((devices,))],
        cost_estimate=build_cost,
        compiler_params=pltpu.CompilerParams(vmem_limit_bytes=max(LIMIT, remote_bytes)),
        name="remote_tiles",
    )(far_work, feature_bands, got_coords, rvec, deg, start_block)

    centre, halfwidth, values = chebyshev_terms()
    flat_shape = jax.ShapeDtypeStruct((vectors, bands * BAND), jnp.float32)
    total_shape = jax.ShapeDtypeStruct((bands, vectors, BAND), jnp.float32)
    gram_shape = jax.ShapeDtypeStruct((devices, 8, vectors * vectors // 8), jnp.float32)
    fetching = [
        work_space,
        pltpu.VMEM((count_all, BAND, BAND), jnp.bfloat16),
        pltpu.SemaphoreType.DMA,
        pltpu.SemaphoreType.DMA((count_all // GROUP,)),
    ]
    product_cost = pl.CostEstimate(
        flops=tile_area * vectors, bytes_accessed=tile_area, transcendentals=0
    )
    previous, current = start_block, start_block
    for power in range(DEGREE):
        first, last = power == 0, power == DEGREE - 1
        if first:
            lead, old = 1.0 / values[1], 0.0
        else:
            lead = 2.0 * values[power] / values[power + 1]
            old = values[power - 1] / values[power + 1]
        gains = (lead * (1.0 - centre) / halfwidth, -lead / halfwidth, old)
        got = exchange(send.reshape(devices, MOST, vectors, BAND)).reshape(entries, vectors, BAND)
        own_total = pl.pallas_call(
            own_kernel,
            out_shape=total_shape,
            in_specs=[whole(pltpu.HBM), whole(), whole(pltpu.HBM)],
            out_specs=whole(),
            scratch_shapes=fetching,
            cost_estimate=product_cost,
            compiler_params=pltpu.CompilerParams(vmem_limit_bytes=LIMIT),
            name="own" + str(power),
        )(near_work, scaled, near_tiles)
        outs = (flat_shape, gram_shape) if last else (flat_shape, row_shape, send_shape)
        results = pl.pallas_call(
            functools.partial(round_kernel, first, last, gains),
            out_shape=outs,
            in_specs=[whole(pltpu.HBM)] + [whole()] * 5 + [whole(pltpu.HBM)],
            out_specs=tuple([whole()] * len(outs)),
            scratch_shapes=[pltpu.VMEM((bands, vectors, BAND), jnp.float32)] + fetching,
            cost_estimate=product_cost,
            compiler_params=pltpu.CompilerParams(vmem_limit_bytes=LIMIT),
            name="round" + str(power),
        )(far_work, got, own_total, root, current, previous, far_tiles)
        previous, current = current, results[0]
        if last:
            parts = exchange(results[1])
        else:
            scaled, send = results[1], results[2]

    basis, factor = pl.pallas_call(
        functools.partial(finish_kernel, devices * bands * BAND),
        out_shape=(flat_shape, jax.ShapeDtypeStruct((vectors, vectors), jnp.float32)),
        in_specs=[whole()] * 2,
        out_specs=(whole(), whole()),
        compiler_params=pltpu.CompilerParams(vmem_limit_bytes=LIMIT),
        name="finish",
    )(parts, current)
    return (basis, factor)


def solution(mesh):
    placed = (P(AXES, None), P(AXES), P(None, AXES), P(AXES, None), P(AXES, None))
    return jax.shard_map(
        on_device,
        mesh=mesh,
        in_specs=placed,
        out_specs=(P(None, AXES), P()),
        check_vma=False,
    )
```

```python
import functools
import math

import jax
import jax.numpy as jnp
from jax import lax
from jax.experimental import pallas as pl
from jax.experimental.pallas import tpu as pltpu
from jax.sharding import PartitionSpec as P

AXES = ("gx", "gy")
BAND = 128
MOST = 2
DEGREE = 4
GROUP = 32
STAGES = 3
EXTRA = 8
AHEAD = 4
LIMIT = 50 * 1024 * 1024

LOW_EDGE = 0.2
HIGH_EDGE = 2.0

VMEM = pltpu.VMEM
SMEM = pltpu.SMEM


def chebyshev_terms():
    centre = 0.5 * (LOW_EDGE + HIGH_EDGE)
    halfwidth = 0.5 * (HIGH_EDGE - LOW_EDGE)
    anchor = -centre / halfwidth
    values = [1.0, anchor]
    for repeat in range(DEGREE - 1):
        values.append(2.0 * anchor * values[-1] - values[-2])
    return (centre, halfwidth, values)


def exchange(blocks):
    return lax.all_to_all(blocks, AXES, split_axis=0, concat_axis=0, tiled=True)


def whole(space=VMEM):
    return pl.BlockSpec(memory_space=space)


def need_kernel(ids, mask, need):
    slots, bands = ids.shape
    devices = need.shape[0]
    device_ids = lax.broadcasted_iota(jnp.int32, (devices, bands), 0)
    band_ids = lax.broadcasted_iota(jnp.int32, (bands, bands), 0)
    owners, withins = [], []
    for j in range(slots):
        row = ids[j : j + 1, :]
        keep = mask[j : j + 1, :] == 1
        owners.append(jnp.where((row // bands == device_ids) & keep, 1.0, 0.0))
        withins.append(jnp.where(row % bands == band_ids, 1.0, 0.0))
    count = lax.dot_general(
        jnp.concatenate(owners, axis=1).astype(jnp.bfloat16),
        jnp.concatenate(withins, axis=1).astype(jnp.bfloat16),
        (((1,), (1,)), ((), ())),
        preferred_element_type=jnp.float32,
    )
    need[...] = jnp.where(count > 0.0, 1, 0).astype(jnp.int32)


def sides_kernel(features, widths, copied, sides, rvec):
    dims = features.shape[2]
    ones = jnp.ones((EXTRA, dims), jnp.bfloat16)
    row = lax.broadcasted_iota(jnp.int32, (EXTRA, BAND), 0)

    def row_sums(part):
        return lax.dot_general(
            ones, part, (((1,), (1,)), ((), ())), preferred_element_type=jnp.float32
        )

    for band in range(features.shape[0]):
        block = features[band]
        for part in range(dims // BAND):
            lanes = slice(part * BAND, (part + 1) * BAND)
            copied[band, lanes, :] = block[:, lanes]
        wide = block.astype(jnp.float32)
        exact = wide * wide
        high = exact.astype(jnp.bfloat16)
        low = (exact - high.astype(jnp.float32)).astype(jnp.bfloat16)
        half = 0.5 * (row_sums(high) + row_sums(low))
        width = jnp.broadcast_to(widths[band : band + 1, :], (EXTRA, BAND))
        product = half * width
        first = product.astype(jnp.bfloat16).astype(jnp.float32)
        left = product - first
        second = left.astype(jnp.bfloat16).astype(jnp.float32)
        third = left - second
        part = row % (EXTRA // MOST)
        side = jnp.where(part == 0, width, first)
        side = jnp.where(part == 2, second, jnp.where(part == 3, third, side))
        sides[band] = side.astype(jnp.bfloat16)
        rvec[band] = jnp.where(row == 0, half, (2.0 * math.log2(math.e)) * width)


def pack_kernel(send_index, features, sides, send, tails, sems):
    devices = send.shape[0]
    depth = features.shape[1]

    def bands_of(d):
        return [
            pltpu.make_async_copy(
                features.at[send_index[d, h]], send.at[d, pl.ds(h * depth, depth)], sems.at[h, d]
            )
            for h in range(MOST)
        ]

    def tail_of(d):
        return pltpu.make_async_copy(
            tails.at[d], send.at[d, pl.ds(MOST * depth, EXTRA)], sems.at[MOST, d]
        )

    def first(d, carry):
        for copy in bands_of(d):
            copy.start()
        row = lax.broadcasted_iota(jnp.int32, (EXTRA, BAND), 0)
        near, far = [sides[send_index[d, h]].astype(jnp.float32) for h in range(MOST)]
        tails[d] = jnp.where(row < EXTRA // MOST, near, far).astype(jnp.bfloat16)
        return carry

    def second(d, carry):
        tail_of(d).start()
        return carry

    def third(d, carry):
        for copy in bands_of(d):
            copy.wait()
        tail_of(d).wait()
        return carry

    lax.fori_loop(0, devices, first, 0, unroll=4)
    lax.fori_loop(0, devices, second, 0, unroll=4)
    lax.fori_loop(0, devices, third, 0, unroll=4)


def spread_column(side, h):
    row = lax.broadcasted_iota(jnp.int32, (EXTRA, 2 * BAND), 0)
    lane = lax.broadcasted_iota(jnp.int32, (EXTRA, 2 * BAND), 1)
    base = h * (EXTRA // MOST)
    left = jnp.where((row == base) & (lane < BAND), 1.0, 0.0)
    right = jnp.where((row > base) & (row < base + 4) & (lane >= BAND), 1.0, 0.0)
    return lax.dot_general(
        side, (left + right).astype(jnp.bfloat16), (((0,), (0,)), ((), ())),
        preferred_element_type=jnp.float32,
    )


def tile_groups(work, rows, coords_of, cols, rvec, tiles, deg, stage, sems, between):
    groups = (work[3, 0] + GROUP - 1) // GROUP

    def copy_of(group):
        slot = lax.rem(group, STAGES)
        return pltpu.make_async_copy(
            stage.at[slot], tiles.at[pl.ds(group * GROUP, GROUP)], sems.at[slot]
        )

    def body(group, carry):
        slot = lax.rem(group, STAGES)

        @pl.when(group >= STAGES)
        def _():
            copy_of(group - STAGES).wait()

        for u in range(GROUP):
            at = group * GROUP + u
            band = work[0, at]
            entry = work[1, at]
            keep = work[2, at].astype(jnp.float32)
            inner = lax.dot_general(
                coords_of(entry), rows[band], (((1,), (1,)), ((), ())),
                preferred_element_type=jnp.float32,
            )
            half_sq = rvec[band, 0:1, :]
            row_width = rvec[band, 1:2, :]
            power = ((inner - half_sq) * cols[entry, :, 0:BAND] - cols[entry, :, BAND:]) * row_width
            weights = jnp.exp2(power) * keep
            stage[slot, u] = weights.astype(jnp.bfloat16)
            deg[band] += jnp.sum(weights.reshape(BAND // 8, 8, BAND), axis=0)
        copy_of(group).start()
        return carry

    lax.fori_loop(0, groups, body, 0)
    between()
    for back in range(STAGES, 0, -1):
        @pl.when(groups >= back)
        def _():
            copy_of(groups - back).wait()


def local_kernel(work, rows, sides, rvec, tiles, deg, cols, stage, sems):
    deg[...] = jnp.zeros(deg.shape, deg.dtype)

    def fill(band, carry):
        cols[band] = spread_column(sides[band], 0)
        return carry

    lax.fori_loop(0, rows.shape[0], fill, 0, unroll=4)
    tile_groups(work, rows, lambda entry: rows[entry], cols, rvec, tiles, deg, stage, sems, lambda: None)


def pack_rows(work, scaled, send):
    def one(at, carry):
        send[at] = scaled[work[4, at]]
        return carry

    lax.fori_loop(0, send.shape[0], one, 0, unroll=8)


def remote_kernel(work_in, rows, got_in, rvec, deg_in, start,
                  tiles, root, scaled, send_out, work, got, deg, send, cols, stage, sems,
                  work_sem, got_sems, send_sem):
    work_copy = pltpu.make_async_copy(work_in, work, work_sem)
    work_copy.start()

    def copy_of(owner):
        return pltpu.make_async_copy(got_in.at[owner], got.at[owner], got_sems.at[owner])

    def begin(owner, carry):
        copy_of(owner).start()
        return carry

    lax.fori_loop(0, got.shape[0], begin, 0)
    deg[...] = deg_in[...]
    halves = rows.shape[2] // BAND
    tail = MOST * halves * BAND
    step = 4

    def fill(part, carry):
        for k in range(step):
            copy_of(part * step + k).wait()
        for k in range(step):
            owner = part * step + k
            for h in range(MOST):
                cols[owner * MOST + h] = spread_column(got[owner, tail : tail + EXTRA, :], h)
        return carry

    lax.fori_loop(0, got.shape[0] // step, fill, 0)
    work_copy.wait()

    def coords_of(entry):
        at = pl.multiple_of(lax.rem(entry, MOST) * (halves * BAND), BAND)
        return jnp.concatenate(
            [got[entry // MOST, pl.ds(at + part * BAND, BAND), :] for part in range(halves)], axis=1
        )

    def between():
        for band in range(deg.shape[0]):
            total = jnp.sum(deg[band], axis=0, keepdims=True)
            inverse = 1.0 / jnp.sqrt(total)
            root[band : band + 1, :] = inverse
            block = start[:, band * BAND : (band + 1) * BAND]
            scaled[band] = (block * inverse).astype(jnp.bfloat16)
        pack_rows(work, scaled, send)
        send_copy.start()

    send_copy = pltpu.make_async_copy(send, send_out, send_sem)
    tile_groups(work, rows, coords_of, cols, rvec, tiles, deg, stage, sems, between)
    send_copy.wait()


def gather_product(work_in, table, tiles, total, work, held, work_sem, sems):
    work_copy = pltpu.make_async_copy(work_in, work, work_sem)

    def copy_of(group):
        part = pl.ds(group * GROUP, GROUP)
        return pltpu.make_async_copy(tiles.at[part], held.at[part], sems.at[group])

    def begin(group, carry):
        copy_of(group).start()
        return carry

    def body(group, carry):
        copy_of(group).wait()
        for u in range(GROUP):
            at = group * GROUP + u
            total[work[0, at]] += jnp.dot(
                table[work[1, at]], held[at], preferred_element_type=jnp.float32
            )
        return carry

    def spare(group, carry):
        copy_of(group).wait()
        return carry

    ahead = min(AHEAD, sems.shape[0])
    work_copy.start()
    for group in range(ahead):
        copy_of(group).start()
    work_copy.wait()
    groups = (work[3, 0] + GROUP - 1) // GROUP
    lax.fori_loop(ahead, groups, begin, 0)
    lax.fori_loop(0, groups, body, 0)
    lax.fori_loop(groups, ahead, spare, 0)


def own_kernel(work_in, scaled, tiles, total, work, held, work_sem, sems):
    total[...] = jnp.zeros(total.shape, total.dtype)
    gather_product(work_in, scaled, tiles, total, work, held, work_sem, sems)


def fold(square):
    return jnp.concatenate([square[8 * q : 8 * q + 8, :] for q in range(square.shape[0] // 8)], axis=1)


def unfold(packed, side):
    return jnp.concatenate([packed[:, side * q : side * (q + 1)] for q in range(side // 8)], axis=0)


def round_kernel(first, last, gains, work_in, got, total_in, root, cur, prev, tiles, following, *rest):
    if last:
        gram, total, work, held, work_sem, sems = rest
    else:
        scaled, send, total, work, held, work_sem, sems = rest
    total[...] = total_in[...]
    gather_product(work_in, got, tiles, total, work, held, work_sem, sems)
    own, mixed_gain, old = gains
    for band in range(total.shape[0]):
        inverse = root[band : band + 1, :]
        lanes = slice(band * BAND, (band + 1) * BAND)
        block = own * cur[:, lanes] + (mixed_gain * inverse) * total[band]
        if not first:
            block = block - old * prev[:, lanes]
        following[:, lanes] = block
        if not last:
            scaled[band] = (inverse * block).astype(jnp.bfloat16)
    if last:
        piece = following[...]
        square = lax.dot_general(
            piece, piece, (((1,), (1,)), ((), ())),
            precision=lax.Precision.HIGHEST, preferred_element_type=jnp.float32,
        )
        gram[...] = jnp.broadcast_to(fold(square)[None], gram.shape)
    else:
        pack_rows(work, scaled, send)


def finish_kernel(total_rows, parts, flat, basis, factor):
    vectors = flat.shape[0]
    gram = unfold(jnp.sum(parts[...], axis=0), vectors) / total_rows
    row_ids = lax.broadcasted_iota(jnp.int32, (vectors, vectors), 0)
    col_ids = lax.broadcasted_iota(jnp.int32, (vectors, vectors), 1)
    left = gram
    right = jnp.where(row_ids == col_ids, 1.0, 0.0).astype(jnp.float32)
    lower = jnp.zeros((vectors, vectors), jnp.float32)
    scale = jnp.zeros((vectors, 1), jnp.float32)
    rows = lax.broadcasted_iota(jnp.int32, (vectors, 1), 0)
    for j in range(vectors):
        pivot = left[j : j + 1, j : j + 1]
        inverse = 1.0 / pivot
        column = left[:, j : j + 1]
        ratio = jnp.where(rows > j, column * inverse, 0.0)
        spread = 1.0 / jnp.sqrt(pivot)
        scale = jnp.where(rows == j, spread, scale)
        lower = jnp.where((col_ids == j) & (row_ids >= j), column * spread, lower)
        left_row = left[j : j + 1, :]
        right_row = right[j : j + 1, :]
        left = left - ratio * left_row
        right = right - ratio * right_row
    factor[...] = lower
    basis[...] = jnp.dot(
        right * scale, flat[...], precision=lax.Precision.HIGHEST, preferred_element_type=jnp.float32
    )


def on_device(features, inv_width, start_block, neighbour_ids, slot_mask):
    bands, slots = neighbour_ids.shape
    dims = features.shape[1]
    vectors = start_block.shape[0]
    devices = lax.axis_size(AXES)
    device = lax.axis_index(AXES)
    entries = devices * MOST
    count_all = bands * slots

    ids = neighbour_ids.T
    mask = slot_mask.T
    need_mine = pl.pallas_call(
        need_kernel,
        out_shape=jax.ShapeDtypeStruct((devices, bands), jnp.int32),
        in_specs=[whole()] * 2,
        out_specs=whole(),
        name="need",
    )(ids, mask)
    wanted = exchange(need_mine)
    rank_send = jnp.cumsum(wanted, axis=1) - 1
    picks = (wanted[:, None, :] == 1) & (
        rank_send[:, None, :] == jnp.arange(MOST, dtype=jnp.int32)[None, :, None]
    )
    send_index = jnp.sum(
        picks.astype(jnp.int32) * jnp.arange(bands, dtype=jnp.int32)[None, None, :], axis=2
    )

    feature_bands = features.reshape(bands, BAND, dims)
    widths = inv_width.reshape(bands, BAND).astype(jnp.float32)
    copied, sides, rvec = pl.pallas_call(
        sides_kernel,
        out_shape=(
            jax.ShapeDtypeStruct((bands, dims, BAND), jnp.bfloat16),
            jax.ShapeDtypeStruct((bands, EXTRA, BAND), jnp.bfloat16),
            jax.ShapeDtypeStruct((bands, EXTRA, BAND), jnp.float32),
        ),
        in_specs=[whole()] * 2,
        out_specs=(whole(), whole(), whole()),
        compiler_params=pltpu.CompilerParams(vmem_limit_bytes=LIMIT),
        cost_estimate=pl.CostEstimate(
            flops=4 * bands * BAND * BAND * dims, bytes_accessed=4 * features.size, transcendentals=0
        ),
        name="sides",
    )(feature_bands, widths)
    send_coords = pl.pallas_call(
        pack_kernel,
        out_shape=jax.ShapeDtypeStruct((devices, MOST * dims + EXTRA, BAND), jnp.bfloat16),
        in_specs=[whole(SMEM)] + [whole()] * 2,
        out_specs=whole(pl.ANY),
        scratch_shapes=[
            pltpu.VMEM((devices, EXTRA, BAND), jnp.bfloat16),
            pltpu.SemaphoreType.DMA((MOST + 1, devices)),
        ],
        compiler_params=pltpu.CompilerParams(vmem_limit_bytes=LIMIT),
        name="pack",
    )(send_index, copied, sides)
    got_coords = exchange(send_coords)

    flat_ids = ids.reshape(-1)
    active = mask.reshape(-1) == 1
    owner_dev = flat_ids // bands
    within = flat_ids % bands
    far = active & (owner_dev != device)
    rank_mine = jnp.cumsum(need_mine, axis=1) - 1
    rank_lookup = jnp.take(rank_mine.reshape(-1), flat_ids, axis=0, mode="clip")
    entry_of = jnp.where(far, owner_dev * MOST + rank_lookup, within)
    order = jnp.arange(count_all, dtype=jnp.int32)

    def work_list(chosen):
        ones = chosen.astype(jnp.int32)
        place = jnp.cumsum(ones) - 1
        hit = ((place[None, :] == order[:, None]) & chosen[None, :]).astype(jnp.int32)
        tile_id = jnp.sum(hit * order[None, :], axis=1)
        entry = jnp.sum(hit * entry_of[None, :], axis=1)
        count = jnp.sum(ones)
        keep = (order < count).astype(jnp.int32)
        rows = jnp.stack([tile_id % bands, entry, keep, jnp.broadcast_to(count, order.shape)])
        rows = jnp.pad(rows, ((0, 0), (0, width - count_all)))
        return jnp.concatenate([rows, send_row], axis=0)

    width = -(-max(count_all, entries) // BAND) * BAND
    send_row = jnp.pad(send_index.reshape(1, entries), ((0, 0), (0, width - entries)))
    near_work = work_list(active & ~far)
    far_work = work_list(far)

    work_space = pltpu.SMEM(far_work.shape, jnp.int32)
    tile_shape = jax.ShapeDtypeStruct((count_all, BAND, BAND), jnp.bfloat16)

    def building(columns):
        return [
            pltpu.VMEM((columns, BAND, 2 * BAND), jnp.float32),
            pltpu.VMEM((STAGES, GROUP, BAND, BAND), jnp.bfloat16),
            pltpu.SemaphoreType.DMA((STAGES,)),
        ]

    remote_bytes = entries * BAND * (8 * BAND + 3 * dims) + 10 * 1024 * 1024
    tile_area = count_all * BAND * BAND
    build_cost = pl.CostEstimate(
        flops=tile_area * dims, bytes_accessed=tile_area, transcendentals=tile_area // 2
    )
    near_tiles, deg = pl.pallas_call(
        local_kernel,
        out_shape=(tile_shape, jax.ShapeDtypeStruct((bands, 8, BAND), jnp.float32)),
        in_specs=[whole(SMEM)] + [whole()] * 3,
        out_specs=(whole(pl.ANY), whole()),
        scratch_shapes=building(bands),
        cost_estimate=build_cost,
        compiler_params=pltpu.CompilerParams(vmem_limit_bytes=LIMIT),
        name="local_tiles",
    )(near_work, feature_bands, sides, rvec)

    row_shape = jax.ShapeDtypeStruct((bands, vectors, BAND), jnp.bfloat16)
    send_shape = jax.ShapeDtypeStruct((entries, vectors, BAND), jnp.bfloat16)
    far_tiles, root, scaled, send = pl.pallas_call(
        remote_kernel,
        out_shape=(tile_shape, jax.ShapeDtypeStruct((bands, BAND), jnp.float32), row_shape, send_shape),
        in_specs=[whole(pltpu.HBM), whole(), whole(pltpu.HBM)] + [whole()] * 3,
        out_specs=(whole(pl.ANY), whole(), whole(), whole(pl.ANY)),
        scratch_shapes=[
            work_space,
            pltpu.VMEM(send_coords.shape, jnp.bfloat16),
            pltpu.VMEM((bands, 8, BAND), jnp.float32),
            pltpu.VMEM(send_shape.shape, jnp.bfloat16),
        ] + building(entries) + [
            pltpu.SemaphoreType.DMA, pltpu.SemaphoreType.DMA((devices,)), pltpu.SemaphoreType.DMA,
        ],
        cost_estimate=build_cost,
        compiler_params=pltpu.CompilerParams(vmem_limit_bytes=max(LIMIT, remote_bytes)),
        name="remote_tiles",
    )(far_work, feature_bands, got_coords, rvec, deg, start_block)

    centre, halfwidth, values = chebyshev_terms()
    flat_shape = jax.ShapeDtypeStruct((vectors, bands * BAND), jnp.float32)
    total_shape = jax.ShapeDtypeStruct((bands, vectors, BAND), jnp.float32)
    gram_shape = jax.ShapeDtypeStruct((devices, 8, vectors * vectors // 8), jnp.float32)
    fetching = [
        work_space,
        pltpu.VMEM((count_all, BAND, BAND), jnp.bfloat16),
        pltpu.SemaphoreType.DMA,
        pltpu.SemaphoreType.DMA((count_all // GROUP,)),
    ]
    product_cost = pl.CostEstimate(
        flops=tile_area * vectors, bytes_accessed=tile_area, transcendentals=0
    )
    previous, current = start_block, start_block
    for power in range(DEGREE):
        first, last = power == 0, power == DEGREE - 1
        if first:
            lead, old = 1.0 / values[1], 0.0
        else:
            lead = 2.0 * values[power] / values[power + 1]
            old = values[power - 1] / values[power + 1]
        gains = (lead * (1.0 - centre) / halfwidth, -lead / halfwidth, old)
        got = exchange(send.reshape(devices, MOST, vectors, BAND)).reshape(entries, vectors, BAND)
        own_total = pl.pallas_call(
            own_kernel,
            out_shape=total_shape,
            in_specs=[whole(pltpu.HBM), whole(), whole(pltpu.HBM)],
            out_specs=whole(),
            scratch_shapes=fetching,
            cost_estimate=product_cost,
            compiler_params=pltpu.CompilerParams(vmem_limit_bytes=LIMIT),
            name="own" + str(power),
        )(near_work, scaled, near_tiles)
        outs = (flat_shape, gram_shape) if last else (flat_shape, row_shape, send_shape)
        results = pl.pallas_call(
            functools.partial(round_kernel, first, last, gains),
            out_shape=outs,
            in_specs=[whole(pltpu.HBM)] + [whole()] * 5 + [whole(pltpu.HBM)],
            out_specs=tuple([whole()] * len(outs)),
            scratch_shapes=[pltpu.VMEM((bands, vectors, BAND), jnp.float32)] + fetching,
            cost_estimate=product_cost,
            compiler_params=pltpu.CompilerParams(vmem_limit_bytes=LIMIT),
            name="round" + str(power),
        )(far_work, got, own_total, root, current, previous, far_tiles)
        previous, current = current, results[0]
        if last:
            parts = exchange(results[1])
        else:
            scaled, send = results[1], results[2]

    basis, factor = pl.pallas_call(
        functools.partial(finish_kernel, devices * bands * BAND),
        out_shape=(flat_shape, jax.ShapeDtypeStruct((vectors, vectors), jnp.float32)),
        in_specs=[whole()] * 2,
        out_specs=(whole(), whole()),
        compiler_params=pltpu.CompilerParams(vmem_limit_bytes=LIMIT),
        name="finish",
    )(parts, current)
    return (basis, factor)


def solution(mesh):
    placed = (P(AXES, None), P(AXES), P(None, AXES), P(AXES, None), P(AXES, None))
    return jax.shard_map(
        on_device,
        mesh=mesh,
        in_specs=placed,
        out_specs=(P(None, AXES), P()),
        check_vma=False,
    )
```
